32 devices in a mesh: batch: 4 (over x, core), lat: 8 (over z, y).
Axes of the slice: x: 2, y: 2, z: 4, core: 2. Of those that a mesh axis runs over, the one named last changes fastest.
Arguments:
- predicted: bfloat16 [4, 73, 192, 1440], P('batch', None, 'lat'), may hold values from -64 to 64
- target: bfloat16 [4, 73, 192, 1440], P('batch', None, 'lat'), may hold values from -128 to 128
- legendre_basis: bfloat16 [192, 96, 720], P(None, ('batch', 'lat')), may hold values from -1 to 1
Outputs:
- spectra: float32 [2, 73, 720], replicated
- channel_loss: float32 [73], replicated
The draws below stay inside these ranges and needn't reach their ends.
All inputs are finite; a program needn't handle non-finite values.
Results may differ from the reference program's by a relative error of at most 0.0003.
Values may be sent and summed in bfloat16 or wider, within the bound.
No kernel may reach another device: no remote copies, remote signals or barrier semaphores. Data moves between devices by JAX's collectives and lax.ppermute only.
A program may use at most 128 MiB of HBM per device.

```python
import math
import jax
import jax.numpy as jnp
from jax import lax

C = 73
NLON = 1440
L = 720
NLAT = 192
BATCH = 4
M = 96


def channel_scales(key):
    base_key = jax.random.fold_in(key, 7001)
    logs = jax.random.uniform(base_key, (C,), jnp.float32, 0.0, 0.6)
    return jnp.exp(logs)


def target_factors(key):
    ratio_key = jax.random.fold_in(key, 7002)
    return jnp.exp(jax.random.uniform(ratio_key, (C,), jnp.float32, -0.7, 0.7))


def field_entries(key, shape):
    return jnp.clip(jax.random.normal(key, shape, jnp.float32), -6.0, 6.0)


def draw_predicted(key, part):
    scales = channel_scales(key)
    values = field_entries(jax.random.fold_in(key, 7003), (BATCH, C, NLAT, NLON))
    return (values * scales[None, :, None, None]).astype(jnp.bfloat16)


def draw_target(key, part):
    scales = channel_scales(key) * target_factors(key)
    values = field_entries(jax.random.fold_in(key, 7004), (BATCH, C, NLAT, NLON))
    return (values * scales[None, :, None, None]).astype(jnp.bfloat16)


def draw_legendre_basis(key, part):
    values = field_entries(jax.random.fold_in(key, 7005), (NLAT, M, L))
    scaled = jnp.clip(values / jnp.sqrt(jnp.float32(NLAT)), -1.0, 1.0)
    return scaled.astype(jnp.bfloat16)


def setup_inputs(seed: int = 0) -> dict:
    splits = jax.random.split(jax.random.key(seed), 4)
    return {
        "predicted": draw_predicted(jax.random.fold_in(splits[3], 71), 0),
        "target": draw_target(jax.random.fold_in(splits[3], 71), 0),
        "legendre_basis": draw_legendre_basis(jax.random.fold_in(splits[3], 71), 0),
    }


def fourier_table():
    lon_ids = jnp.arange(NLON, dtype=jnp.int32)
    order_ids = jnp.arange(M, dtype=jnp.int32)
    product_ids = lon_ids[:, None] * order_ids[None, :] % NLON
    angles = 2.0 * math.pi / NLON * product_ids.astype(jnp.float32)
    inv_root = 1.0 / math.sqrt(NLON)
    return jnp.stack([jnp.cos(angles) * inv_root, -jnp.sin(angles) * inv_root], axis=1).astype(jnp.bfloat16)

def reference(predicted, target, legendre_basis):
    dft_table = fourier_table().astype(jnp.float32)
    basis_wide = legendre_basis.astype(jnp.float32)
    order_ids = jnp.arange(M, dtype=jnp.int32)
    weights = jnp.where(order_ids == 0, 1.0, 2.0).astype(jnp.float32)

    def member_energy(field_in):
        fourier = jnp.einsum('cnk,kpm->pmcn', field_in.astype(jnp.float32), dft_table).astype(jnp.bfloat16)
        coefficients = jnp.einsum('pmcn,nml->pmcl', fourier.astype(jnp.float32), basis_wide)
        squares = lax.optimization_barrier(jnp.sum(coefficients * coefficients, axis=0))
        return lax.optimization_barrier(jnp.sum(squares * weights[:, None, None], axis=0))
    energy_pred = lax.optimization_barrier(jnp.sum(lax.map(member_energy, predicted), axis=0))
    energy_target = lax.optimization_barrier(jnp.sum(lax.map(member_energy, target), axis=0))
    spectra = jnp.stack([energy_pred, energy_target], axis=0) / (BATCH * M)
    log_spectra = jnp.log(spectra + 1e-06)
    channel_loss = lax.optimization_barrier(jnp.mean((log_spectra[0] - log_spectra[1]) ** 2, axis=1))
    return (spectra, channel_loss)
```

```python
import functools
import math

import jax
import jax.numpy as jnp
import numpy as np
from jax import lax
from jax.experimental import pallas as pl
from jax.experimental.pallas import tpu as pltpu
from jax.sharding import PartitionSpec as P

LANES = 128
VMEM_LIMIT = 60 * 1024 * 1024


def round_up(value, step):
    return -(-value // step) * step


def fourier_table(lon_count, groups, bands, per_dev):
    orders = np.arange(groups * bands * per_dev).reshape(groups, bands, per_dev)
    orders = orders.transpose(1, 0, 2).reshape(-1)
    product_ids = np.arange(lon_count)[:, None] * orders[None, :] % lon_count
    angles = np.float32(2.0 * math.pi / lon_count) * product_ids.astype(np.float32)
    inv_root = np.float32(1.0 / math.sqrt(lon_count))
    both = np.stack([np.cos(angles) * inv_root, -np.sin(angles) * inv_root], axis=2)
    flat = both.reshape(lon_count, -1).astype(jnp.bfloat16)
    padded = round_up(flat.shape[1], LANES)
    return np.pad(flat, ((0, 0), (0, padded - flat.shape[1])))


def peers(count, step):
    if count & (count - 1) == 0:
        return [(i, i ^ step) for i in range(count)]
    return [(i, (i + step) % count) for i in range(count)]


def target_of(index, count, step):
    if count & (count - 1) == 0:
        return jnp.bitwise_xor(index, step)
    return lax.rem(index + step, count)


def source_of(index, count, step):
    if count & (count - 1) == 0:
        return jnp.bitwise_xor(index, step)
    return lax.rem(index + count - step, count)


def dft_kernel(bands, per, chans, lats, chunks, place, p_hbm, t_hbm, table, *rest):
    outs = rest[:bands]
    xbuf, dscr, turned, packed, sems = rest[bands:]
    copies = []
    for f, field in enumerate((p_hbm, t_hbm)):
        row = 0
        for i, rows in enumerate(chunks):
            cp = pltpu.make_async_copy(
                field.at[pl.ds(row, rows), :], xbuf.at[f, pl.ds(row, rows), :], sems.at[f, i]
            )
            cp.start()
            copies.append((f, row, rows, cp))
            row += rows
    band = place[0]
    tiles = dscr.shape[0]
    for f in range(2):
        for owner, row, rows, cp in copies:
            if owner != f:
                continue
            cp.wait()
            res = jnp.dot(
                xbuf[f, pl.ds(row, rows), :], table[...], preferred_element_type=jnp.float32
            )
            for q in range(tiles):
                dscr[q, pl.ds(row, rows), :] = res[:, q * LANES : (q + 1) * LANES]

        def turn(q, carry):
            for n in range(lats):
                block = dscr.at[q][pl.ds(n, LANES, stride=lats), :]
                turned.at[q][pl.ds(n, LANES, stride=lats), :] = block.T
            return carry

        lax.fori_loop(0, tiles, turn, 0)

        def pack(s, carry):
            base = target_of(band, bands, s) * per
            for g in range(per):
                column = base + g
                start = pl.multiple_of(lax.rem(column, LANES) * lats, 8)
                packed[s, :, pl.ds(g * chans, chans)] = turned[
                    column // LANES, pl.ds(start, lats), pl.ds(0, chans)
                ]
            return carry

        lax.fori_loop(0, bands, pack, 0)
        for s in range(bands):
            outs[s][f] = packed[s].astype(jnp.bfloat16)


def dft_blocks(place, predicted, target, table, bands, per, chans, lats):
    rows_all, lon_count = predicted.shape
    width = round_up(per * chans, LANES)
    step = -(-chans // 4) * lats
    chunks = []
    left = rows_all
    while left > 0:
        chunks.append(min(step, left))
        left -= step
    columns = table.shape[1]
    anywhere = pl.BlockSpec(memory_space=pl.ANY)
    vmem = pl.BlockSpec(memory_space=pltpu.VMEM)
    return pl.pallas_call(
        functools.partial(dft_kernel, bands, per, chans, lats, tuple(chunks)),
        out_shape=[jax.ShapeDtypeStruct((2, lats, width), jnp.bfloat16)] * bands,
        in_specs=[pl.BlockSpec(memory_space=pltpu.SMEM), anywhere, anywhere, vmem],
        out_specs=[vmem] * bands,
        scratch_shapes=[
            pltpu.VMEM((2, rows_all, lon_count), jnp.bfloat16),
            pltpu.VMEM((columns // LANES, LANES * lats, LANES), jnp.float32),
            pltpu.VMEM((columns // LANES, LANES * lats, LANES), jnp.float32),
            pltpu.VMEM((bands, lats, width), jnp.float32),
            pltpu.SemaphoreType.DMA((2, len(chunks))),
        ],
        compiler_params=pltpu.CompilerParams(vmem_limit_bytes=VMEM_LIMIT),
        name="dft",
    )(place, predicted, target, table)


def turn_kernel(basis, out):
    for o in range(basis.shape[0]):
        out[o] = basis[o].T


def turned_basis(basis):
    per_dev, lat_count, degrees = basis.shape
    return pl.pallas_call(
        turn_kernel,
        out_shape=jax.ShapeDtypeStruct((per_dev, degrees, lat_count), basis.dtype),
        compiler_params=pltpu.CompilerParams(vmem_limit_bytes=VMEM_LIMIT),
        name="turn",
    )(basis)


def legendre_kernel(bands, groups, per_dev, chans, lats, place, *rest):
    blocks = rest[:bands]
    bases = rest[bands : bands + groups]
    out = rest[bands + groups]
    basis, fourier, columns, total, sems = rest[bands + groups + 1 :]
    band, group = place[0], place[1]
    copies = []
    for q in range(groups):
        start = source_of(group, groups, q) * per_dev
        cp = pltpu.make_async_copy(bases[q], basis.at[pl.ds(start, per_dev)], sems.at[q])
        cp.start()
        copies.append(cp)
    degrees = basis.shape[1]
    width = 2 * chans
    first = jnp.where(band == 0, 1.0, 2.0).astype(jnp.float32)
    for f in range(2):
        for s in range(bands):
            row = pl.multiple_of(source_of(band, bands, s) * lats, 8)
            fourier[pl.ds(row, lats), :] = blocks[s][f].astype(jnp.float32)
        if f == 0:
            for cp in copies:
                cp.wait()
        for i in range(groups * per_dev):
            columns[i] = fourier[:, pl.ds(i * width, width)].astype(jnp.bfloat16)
        coef = jnp.dot(basis[0], columns[0], preferred_element_type=jnp.float32)
        total[:, pl.ds(0, width)] = coef * coef * first

        def one_order(i, carry):
            coef = jnp.dot(basis[i], columns[i], preferred_element_type=jnp.float32)
            total[:, pl.ds(0, width)] += coef * coef * 2.0
            return carry

        lax.fori_loop(1, groups * per_dev, one_order, 0)
        sums = total[...]
        energy = sums[:, :chans] + sums[:, chans:width]
        flat = jnp.pad(
            energy, ((0, round_up(degrees, LANES) - degrees), (0, round_up(chans, 8) - chans))
        )
        lane_tiles = round_up(degrees, LANES) // LANES
        row_tiles = round_up(chans, 8) // 8
        for k in range(lane_tiles):
            piece = flat[k * LANES : (k + 1) * LANES, :].T
            for r in range(row_tiles):
                out[(f * row_tiles + r) * lane_tiles + k] = piece[r * 8 : (r + 1) * 8, :]


def legendre_energy(place, blocks, bases, chans, lats):
    bands, groups = len(blocks), len(bases)
    per_dev, degrees, lat_count = bases[0].shape
    vmem = pl.BlockSpec(memory_space=pltpu.VMEM)
    anywhere = pl.BlockSpec(memory_space=pl.ANY)
    row_tiles = round_up(chans, 8) // 8
    lane_tiles = round_up(degrees, LANES) // LANES
    return pl.pallas_call(
        functools.partial(legendre_kernel, bands, groups, per_dev, chans, lats),
        out_shape=jax.ShapeDtypeStruct((2 * row_tiles * lane_tiles, 8, LANES), jnp.float32),
        in_specs=[pl.BlockSpec(memory_space=pltpu.SMEM)] + [vmem] * bands + [anywhere] * groups,
        out_specs=vmem,
        scratch_shapes=[
            pltpu.VMEM((groups * per_dev, degrees, lat_count), jnp.bfloat16),
            pltpu.VMEM((lat_count, blocks[0].shape[2]), jnp.float32),
            pltpu.VMEM((groups * per_dev, lat_count, 2 * chans), jnp.bfloat16),
            pltpu.VMEM((degrees, round_up(2 * chans, LANES)), jnp.float32),
            pltpu.SemaphoreType.DMA((groups,)),
        ],
        compiler_params=pltpu.CompilerParams(vmem_limit_bytes=VMEM_LIMIT),
        name="legendre",
    )(place, *blocks, *bases)


def loss_kernel(chans, degrees, count, blocks, spectra, loss):
    lane_tiles = round_up(degrees, LANES) // LANES
    row_tiles = round_up(chans, 8) // 8
    scale = 1.0 / count
    for r in range(row_tiles):
        rows = min(8, chans - r * 8)
        acc = jnp.zeros((8, LANES), jnp.float32)
        for k in range(lane_tiles):
            lanes = min(LANES, degrees - k * LANES)
            first = blocks[r * lane_tiles + k] * scale
            second = blocks[(row_tiles + r) * lane_tiles + k] * scale
            spectra[0, pl.ds(r * 8, rows), pl.ds(k * LANES, lanes)] = first[:rows, :lanes]
            spectra[1, pl.ds(r * 8, rows), pl.ds(k * LANES, lanes)] = second[:rows, :lanes]
            gap = jnp.log(first + 1e-06) - jnp.log(second + 1e-06)
            gap = gap * gap
            if lanes < LANES:
                lane_ids = lax.broadcasted_iota(jnp.int32, gap.shape, 1)
                gap = jnp.where(lane_ids < lanes, gap, 0.0)
            acc = acc + gap
        loss[pl.ds(r * 8, 8), :] = jnp.sum(acc, axis=1, keepdims=True) * (1.0 / degrees)


def loss_call(blocks, chans, degrees, count):
    return pl.pallas_call(
        functools.partial(loss_kernel, chans, degrees, count),
        out_shape=(
            jax.ShapeDtypeStruct((2, chans, degrees), jnp.float32),
            jax.ShapeDtypeStruct((round_up(chans, 8), 1), jnp.float32),
        ),
        compiler_params=pltpu.CompilerParams(vmem_limit_bytes=VMEM_LIMIT),
        name="loss",
    )(blocks)


def exchange(value, axis, step):
    return lax.ppermute(value, axis, peers(lax.axis_size(axis), step))


def reduce_all(value):
    halved = []
    for axis in ("batch", "lat"):
        index = lax.axis_index(axis)
        step = 1
        while step < lax.axis_size(axis):
            if value.shape[0] % 2 == 0:
                half = value.shape[0] // 2
                high = (index // step) % 2 == 1
                lower, upper = value[:half], value[half:]
                kept = jnp.where(high, upper, lower)
                sent = jnp.where(high, lower, upper)
                value = kept + exchange(sent, axis, step)
                halved.append((axis, step, high))
            else:
                value = value + exchange(value, axis, step)
            step *= 2
    for axis, step, high in reversed(halved):
        other = exchange(value, axis, step)
        value = jnp.where(
            high, jnp.concatenate([other, value]), jnp.concatenate([value, other])
        )
    return value


def body(predicted, target, legendre_basis):
    groups = lax.axis_size("batch")
    bands = lax.axis_size("lat")
    per_dev = legendre_basis.shape[1]
    members, chans, lats, lon_count = predicted.shape
    degrees = legendre_basis.shape[2]
    place = jnp.stack([lax.axis_index("lat"), lax.axis_index("batch")]).astype(jnp.int32)
    table = jnp.asarray(fourier_table(lon_count, groups, bands, per_dev))
    rows = members * chans * lats
    blocks = dft_blocks(
        place,
        predicted.reshape(rows, lon_count),
        target.reshape(rows, lon_count),
        table,
        bands,
        groups * per_dev * 2,
        chans,
        lats,
    )
    mine = turned_basis(jnp.transpose(legendre_basis, (1, 0, 2)))
    bases = [mine] + [exchange(mine, "batch", q) for q in range(1, groups)]
    arrived = [blocks[0]] + [exchange(blocks[s], "lat", s) for s in range(1, bands)]
    energy = legendre_energy(place, arrived, bases, chans, lats)
    energy = reduce_all(energy)
    spectra, loss = loss_call(energy, chans, degrees, members * groups * groups * bands * per_dev)
    return (spectra, loss[:chans, 0])


def solution(mesh):
    placed = (
        P("batch", None, "lat", None),
        P("batch", None, "lat", None),
        P(None, ("batch", "lat"), None),
    )
    return jax.shard_map(body, mesh=mesh, in_specs=placed, out_specs=(P(), P()), check_vma=False)
```

```python
import functools
import math

import jax
import jax.numpy as jnp
import numpy as np
from jax import lax
from jax.experimental import pallas as pl
from jax.experimental.pallas import tpu as pltpu
from jax.sharding import PartitionSpec as P


LANES = 128
VMEM_LIMIT = 24 * 1024 * 1024
STAGED_LIMIT = 59 * 1024 * 1024
SPARE_VMEM = 16 * 1024 * 1024


def round_up(value, step):
    return -(-value // step) * step


def fourier_table(lon_count, groups, bands, per_dev):
    orders = np.arange(groups * bands * per_dev).reshape(groups, bands, per_dev)
    orders = orders.transpose(1, 0, 2).reshape(-1)
    product_ids = np.arange(lon_count)[:, None] * orders[None, :] % lon_count
    angles = np.float32(2.0 * math.pi / lon_count) * product_ids.astype(np.float32)
    inv_root = np.float32(1.0 / math.sqrt(lon_count))
    both = np.stack([np.cos(angles) * inv_root, -np.sin(angles) * inv_root], axis=2)
    flat = both.reshape(lon_count, -1).astype(jnp.bfloat16)
    padded = round_up(flat.shape[1], LANES)
    return np.pad(flat, ((0, 0), (0, padded - flat.shape[1])))


def peers(count, step):
    if count & (count - 1) == 0:
        return [(i, i ^ step) for i in range(count)]
    return [(i, (i + step) % count) for i in range(count)]


def target_of(index, count, step):
    if count & (count - 1) == 0:
        return jnp.bitwise_xor(index, step)
    return lax.rem(index + step, count)


def source_of(index, count, step):
    if count & (count - 1) == 0:
        return jnp.bitwise_xor(index, step)
    return lax.rem(index + count - step, count)


def dft_kernel(bands, per, chans, lats, chunks, staged, place, field, table, *rest):
    outs = rest[:bands]
    dscr, turned, packed = rest[bands : bands + 3]
    copies = []
    row = 0
    xbuf = rest[bands + 3] if staged else field
    for i, rows in enumerate(chunks):
        cp = None
        if staged:
            cp = pltpu.make_async_copy(
                field.at[pl.ds(row, rows), :], xbuf.at[pl.ds(row, rows), :], rest[-1].at[i]
            )
            cp.start()
        copies.append((row, rows, cp))
        row += rows
    band = place[0]
    tiles = dscr.shape[0]
    for row, rows, cp in copies:
        if staged:
            cp.wait()
        res = jnp.dot(xbuf[pl.ds(row, rows), :], table[...], preferred_element_type=jnp.float32)
        for q in range(tiles):
            dscr[q, pl.ds(row, rows), :] = res[:, q * LANES : (q + 1) * LANES]

    def turn(q, carry):
        for n in range(lats):
            block = dscr.at[q][pl.ds(n, LANES, stride=lats), :]
            turned.at[q][pl.ds(n, LANES, stride=lats), :] = block.T
        return carry

    lax.fori_loop(0, tiles, turn, 0)

    def pack(s, carry):
        base = target_of(band, bands, s) * per
        for g in range(per):
            column = base + g
            start = pl.multiple_of(lax.rem(column, LANES) * lats, 8)
            packed[s, :, pl.ds(g * chans, chans)] = turned[
                column // LANES, pl.ds(start, lats), pl.ds(0, chans)
            ]
        return carry

    lax.fori_loop(0, bands, pack, 0)
    for s in range(bands):
        outs[s][...] = packed[s].astype(jnp.bfloat16)


def dft_blocks(place, field, table, bands, per, chans, lats, staged):
    rows_all, lon_count = field.shape
    width = round_up(per * chans, LANES)
    step = -(-chans // 4) * lats
    chunks = []
    left = rows_all
    while left > 0:
        chunks.append(min(step, left))
        left -= step
    columns = table.shape[1]
    held = 4 * lats * (2 * columns * LANES + bands * width)
    anywhere = pl.BlockSpec(memory_space=pl.ANY)
    vmem = pl.BlockSpec(memory_space=pltpu.VMEM)
    return pl.pallas_call(
        functools.partial(dft_kernel, bands, per, chans, lats, tuple(chunks), staged),
        out_shape=[jax.ShapeDtypeStruct((lats, width), jnp.bfloat16)] * bands,
        in_specs=[pl.BlockSpec(memory_space=pltpu.SMEM), anywhere if staged else vmem, vmem],
        out_specs=[vmem] * bands,
        scratch_shapes=[
            pltpu.VMEM((columns // LANES, LANES * lats, LANES), jnp.float32),
            pltpu.VMEM((columns // LANES, LANES * lats, LANES), jnp.float32),
            pltpu.VMEM((bands, lats, width), jnp.float32),
        ]
        + (
            [
                pltpu.VMEM((rows_all, lon_count), jnp.bfloat16),
                pltpu.SemaphoreType.DMA((len(chunks),)),
            ]
            if staged
            else []
        ),
        compiler_params=pltpu.CompilerParams(
            vmem_limit_bytes=STAGED_LIMIT if staged else SPARE_VMEM + held
        ),
        name="dft",
    )(place, field, table)


def turn_kernel(basis, out):
    for o in range(basis.shape[0]):
        out[o, :, : basis.shape[1]] = basis[o].T


def turned_basis(basis):
    per_dev, lat_count, degrees = basis.shape
    return pl.pallas_call(
        turn_kernel,
        out_shape=jax.ShapeDtypeStruct((per_dev, degrees, round_up(lat_count, LANES)), basis.dtype),
        compiler_params=pltpu.CompilerParams(vmem_limit_bytes=VMEM_LIMIT),
        name="turn",
    )(basis)


def legendre_kernel(bands, groups, per_dev, chans, lats, slots, place, *rest):
    blocks = rest[:bands]
    bases = rest[bands : bands + groups]
    out = rest[bands + groups]
    fourier, columns, total = rest[bands + groups + 1 :]
    band, group = place[0], place[1]
    degrees = bases[0].shape[1]
    depth = bands * lats
    width = 2 * chans
    for s in range(bands):
        row = pl.multiple_of(source_of(band, bands, s) * lats, 8)
        fourier[pl.ds(row, lats), :] = blocks[s][...].astype(jnp.float32)
    for i in range(groups * per_dev):
        columns[i] = fourier[:, pl.ds(i * width, width)].astype(jnp.bfloat16)
    for q in range(groups):
        owner = jnp.bitwise_xor(group, slots[q])
        first = jnp.where(jnp.logical_and(band == 0, owner == 0), 1.0, 2.0)
        squares = None
        for o in range(per_dev):
            coef = jnp.dot(
                bases[q][o, :, :depth],
                columns[owner * per_dev + o],
                preferred_element_type=jnp.float32,
            )
            term = coef * coef * (first if o == 0 else 2.0)
            squares = term if squares is None else squares + term
        if q == 0:
            total[:, pl.ds(0, width)] = squares
        else:
            total[:, pl.ds(0, width)] += squares
    sums = total[...]
    energy = sums[:, :chans] + sums[:, chans:width]
    flat = jnp.pad(
        energy, ((0, round_up(degrees, LANES) - degrees), (0, round_up(chans, 8) - chans))
    )
    lane_tiles = round_up(degrees, LANES) // LANES
    row_tiles = round_up(chans, 8) // 8
    for k in range(lane_tiles):
        piece = flat[k * LANES : (k + 1) * LANES, :].T
        for r in range(row_tiles):
            out[r * lane_tiles + k] = piece[r * 8 : (r + 1) * 8, :]


def legendre_energy(place, blocks, bases, slots, chans, lats):
    bands, groups = len(blocks), len(bases)
    per_dev, degrees, _ = bases[0].shape
    vmem = pl.BlockSpec(memory_space=pltpu.VMEM)
    row_tiles = round_up(chans, 8) // 8
    lane_tiles = round_up(degrees, LANES) // LANES
    return pl.pallas_call(
        functools.partial(legendre_kernel, bands, groups, per_dev, chans, lats, slots),
        out_shape=jax.ShapeDtypeStruct((row_tiles * lane_tiles, 8, LANES), jnp.float32),
        in_specs=[pl.BlockSpec(memory_space=pltpu.SMEM)] + [vmem] * (bands + groups),
        out_specs=vmem,
        scratch_shapes=[
            pltpu.VMEM((bands * lats, blocks[0].shape[1]), jnp.float32),
            pltpu.VMEM((groups * per_dev, bands * lats, 2 * chans), jnp.bfloat16),
            pltpu.VMEM((degrees, round_up(2 * chans, LANES)), jnp.float32),
        ],
        compiler_params=pltpu.CompilerParams(vmem_limit_bytes=VMEM_LIMIT),
        name="legendre",
    )(place, *blocks, *bases)


def loss_kernel(chans, degrees, count, blocks, spectra, loss, sums):
    lane_tiles = round_up(degrees, LANES) // LANES
    row_tiles = round_up(chans, 8) // 8
    scale = 1.0 / count
    for r in range(row_tiles):
        rows = min(8, chans - r * 8)
        acc = jnp.zeros((8, LANES), jnp.float32)
        for k in range(lane_tiles):
            lanes = min(LANES, degrees - k * LANES)
            first = blocks[r * lane_tiles + k] * scale
            second = blocks[(row_tiles + r) * lane_tiles + k] * scale
            spectra[0, pl.ds(r * 8, rows), pl.ds(k * LANES, lanes)] = first[:rows, :lanes]
            spectra[1, pl.ds(r * 8, rows), pl.ds(k * LANES, lanes)] = second[:rows, :lanes]
            gap = jnp.log(first + 1e-06) - jnp.log(second + 1e-06)
            gap = gap * gap
            if lanes < LANES:
                lane_ids = lax.broadcasted_iota(jnp.int32, gap.shape, 1)
                gap = jnp.where(lane_ids < lanes, gap, 0.0)
            acc = acc + gap
        sums[pl.ds(r * 8, 8), :] = acc
    turned = sums[...].T
    loss[...] = (jnp.sum(turned, axis=0, keepdims=True) * (1.0 / degrees))[:, :chans]


def loss_call(blocks, chans, degrees, count):
    return pl.pallas_call(
        functools.partial(loss_kernel, chans, degrees, count),
        out_shape=(
            jax.ShapeDtypeStruct((2, chans, degrees), jnp.float32),
            jax.ShapeDtypeStruct((1, chans), jnp.float32),
        ),
        scratch_shapes=[pltpu.VMEM((round_up(chans, 8), LANES), jnp.float32)],
        compiler_params=pltpu.CompilerParams(vmem_limit_bytes=VMEM_LIMIT),
        name="loss",
    )(blocks)


def exchange(value, axis, step):
    return lax.ppermute(value, axis, peers(lax.axis_size(axis), step))


def reduce_all(value):
    halved = []
    index = lax.axis_index("batch")
    step = 1
    while step < lax.axis_size("batch"):
        if value.shape[0] % 2 == 0:
            half = value.shape[0] // 2
            high = (index // step) % 2 == 1
            lower, upper = value[:half], value[half:]
            kept = jnp.where(high, upper, lower)
            sent = jnp.where(high, lower, upper)
            value = kept + exchange(sent, "batch", step)
            halved.append((step, high))
        else:
            value = value + exchange(value, "batch", step)
        step *= 2
    bands = lax.axis_size("lat")
    step = 1
    radix = 2 if bands.bit_length() % 2 == 0 else 4
    while step < bands:
        parts = [exchange(value, "lat", k * step) for k in range(radix - 1, 0, -1)]
        value = value + sum(parts[1:], parts[0])
        step *= radix
        radix = 4
    for step, high in reversed(halved):
        other = exchange(value, "batch", step)
        value = jnp.where(
            high, jnp.concatenate([other, value]), jnp.concatenate([value, other])
        )
    return value


def spectrum_loss(predicted, target, legendre_basis):
    groups = lax.axis_size("batch")
    bands = lax.axis_size("lat")
    per_dev = legendre_basis.shape[1]
    members, chans, lats, lon_count = predicted.shape
    degrees = legendre_basis.shape[2]
    place = jnp.stack([lax.axis_index("lat"), lax.axis_index("batch")]).astype(jnp.int32)
    table = jnp.asarray(fourier_table(lon_count, groups, bands, per_dev))
    rows = members * chans * lats
    fields = (predicted, target)
    steps = list(range(bands - 1, 0, -1))

    sent = []
    for f, field in enumerate(fields):
        flat = field.reshape(rows, lon_count)
        sent.append(
            dft_blocks(
                place, flat, table, bands, groups * per_dev * 2, chans, lats, f == 0
            )
        )
    arrived = []
    for f in range(2):
        got = {0: sent[f][0]}
        for s in steps:
            got[s] = exchange(sent[f][s], "lat", s)
        arrived.append([got[s] for s in range(bands)])
    bases = [turned_basis(jnp.transpose(legendre_basis, (1, 0, 2)))]
    slots = [0]
    step = groups // 2
    while step:
        bases = bases + [exchange(block, "batch", step) for block in bases]
        slots = slots + [slot ^ step for slot in slots]
        step //= 2
    energies = []
    for f in range(2):
        energies.append(legendre_energy(place, arrived[f], bases, slots, chans, lats))
    energy = reduce_all(jnp.concatenate(energies))
    spectra, loss = loss_call(energy, chans, degrees, members * groups * groups * bands * per_dev)
    return (spectra, loss.reshape(chans))


def solution(mesh):
    placed = (
        P("batch", None, "lat", None),
        P("batch", None, "lat", None),
        P(None, ("batch", "lat"), None),
    )
    return jax.shard_map(spectrum_loss, mesh=mesh, in_specs=placed, out_specs=(P(), P()), check_vma=False)
```

```python
import functools
import math

import jax
import jax.numpy as jnp
import numpy as np
from jax import lax
from jax.experimental import pallas as pl
from jax.experimental.pallas import tpu as pltpu
from jax.sharding import PartitionSpec as P


LANES = 128
VMEM_LIMIT = 24 * 1024 * 1024
STAGED_LIMIT = 59 * 1024 * 1024


def round_up(value, step):
    return -(-value // step) * step


def fourier_table(lon_count, groups, bands, per_dev):
    orders = np.arange(groups * bands * per_dev).reshape(groups, bands, per_dev)
    orders = orders.transpose(1, 0, 2).reshape(-1)
    product_ids = np.arange(lon_count)[:, None] * orders[None, :] % lon_count
    angles = np.float32(2.0 * math.pi / lon_count) * product_ids.astype(np.float32)
    inv_root = np.float32(1.0 / math.sqrt(lon_count))
    both = np.stack([np.cos(angles) * inv_root, -np.sin(angles) * inv_root], axis=2)
    flat = both.reshape(lon_count, -1).astype(jnp.bfloat16)
    padded = round_up(flat.shape[1], LANES)
    return np.pad(flat, ((0, 0), (0, padded - flat.shape[1])))


def peers(count, step):
    if count & (count - 1) == 0:
        return [(i, i ^ step) for i in range(count)]
    return [(i, (i + step) % count) for i in range(count)]


def target_of(index, count, step):
    if count & (count - 1) == 0:
        return jnp.bitwise_xor(index, step)
    return lax.rem(index + step, count)


def source_of(index, count, step):
    if count & (count - 1) == 0:
        return jnp.bitwise_xor(index, step)
    return lax.rem(index + count - step, count)


def dft_kernel(bands, per, chans, lats, chunks, joined, field, table_hbm, *rest):
    near = bands // 2 - 1 if joined else 0
    before, rest = rest[:near], rest[near:]
    outs = rest[:bands]
    dscr, turned, packed, xbuf, table, sems = rest[bands:]
    load = pltpu.make_async_copy(table_hbm, table, sems.at[len(chunks)])
    load.start()
    copies = []
    row = 0
    for i, rows in enumerate(chunks):
        cp = pltpu.make_async_copy(
            field.at[pl.ds(row, rows), :], xbuf.at[pl.ds(row, rows), :], sems.at[i]
        )
        cp.start()
        copies.append((row, rows, cp))
        row += rows
    band = lax.axis_index("lat")
    tiles = dscr.shape[0]
    load.wait()
    for row, rows, cp in copies:
        cp.wait()
        res = jnp.dot(xbuf[pl.ds(row, rows), :], table[...], preferred_element_type=jnp.float32)
        for q in range(tiles):
            dscr[q, pl.ds(row, rows), :] = res[:, q * LANES : (q + 1) * LANES]

    def turn(q, carry):
        for n in range(lats):
            block = dscr.at[q][pl.ds(n, LANES, stride=lats), :]
            turned.at[q][pl.ds(n, LANES, stride=lats), :] = block.T
        return carry

    lax.fori_loop(0, tiles, turn, 0)

    def pack(s, carry):
        base = target_of(band, bands, s) * per
        for g in range(per):
            column = base + g
            start = pl.multiple_of(lax.rem(column, LANES) * lats, 8)
            packed[s, :, pl.ds(g * chans, chans)] = turned[
                column // LANES, pl.ds(start, lats), pl.ds(0, chans)
            ]
        return carry

    lax.fori_loop(0, bands, pack, 0, unroll=min(bands, 8))
    for s in range(bands):
        if 0 < s <= near:
            outs[s][0] = before[s - 1][...]
            outs[s][1] = packed[s].astype(jnp.bfloat16)
        else:
            outs[s][...] = packed[s].astype(jnp.bfloat16)


def dft_blocks(field, table, before, bands, per, chans, lats):
    rows_all, lon_count = field.shape
    width = round_up(per * chans, LANES)
    step = -(-chans // 3) * lats
    chunks = []
    left = rows_all
    while left > 0:
        chunks.append(min(step, left))
        left -= step
    columns = table.shape[1]
    anywhere = pl.BlockSpec(memory_space=pl.ANY)
    vmem = pl.BlockSpec(memory_space=pltpu.VMEM)
    one, two = ((2,) * k + (lats, width) for k in (0, 1))
    out_shape = [
        jax.ShapeDtypeStruct(two if 0 < s <= len(before) else one, jnp.bfloat16)
        for s in range(bands)
    ]
    args = [field, table, *before]
    return pl.pallas_call(
        functools.partial(dft_kernel, bands, per, chans, lats, tuple(chunks), bool(before)),
        out_shape=out_shape,
        in_specs=[anywhere, anywhere] + [vmem] * (len(args) - 2),
        out_specs=[vmem] * len(out_shape),
        scratch_shapes=[
            pltpu.VMEM((columns // LANES, LANES * lats, LANES), jnp.float32),
            pltpu.VMEM((columns // LANES, LANES * lats, LANES), jnp.float32),
            pltpu.VMEM((bands, lats, width), jnp.float32),
            pltpu.VMEM((rows_all, lon_count), jnp.bfloat16),
            pltpu.VMEM(table.shape, jnp.bfloat16),
            pltpu.SemaphoreType.DMA((len(chunks) + 1,)),
        ],
        compiler_params=pltpu.CompilerParams(vmem_limit_bytes=STAGED_LIMIT),
        name="dft",
    )(*args)


def turn_kernel(count, *refs):
    for basis, out in zip(refs[:count], refs[count:]):
        for o in range(basis.shape[0]):
            out[o, :, : basis.shape[1]] = basis[o].T


def turned_bases(bases):
    per_dev, lat_count, degrees = bases[0].shape
    shape = (per_dev, degrees, round_up(lat_count, LANES))
    return pl.pallas_call(
        functools.partial(turn_kernel, len(bases)),
        out_shape=[jax.ShapeDtypeStruct(shape, bases[0].dtype)] * len(bases),
        compiler_params=pltpu.CompilerParams(vmem_limit_bytes=VMEM_LIMIT),
        name="turn",
    )(*bases)


def legendre_kernel(bands, groups, per_dev, chans, lats, slots, field, *rest):
    blocks = rest[:bands]
    bases = rest[bands : bands + groups]
    rest = rest[bands + groups :]
    fourier, columns, total = rest[-3:]
    if field == 0:
        out = rest[0]
    else:
        energy_before, kept, sent, out = rest[0], rest[1], rest[2], rest[3]
    band, group = lax.axis_index("lat"), lax.axis_index("batch")
    degrees = bases[0].shape[1]
    depth = bands * lats
    width = 2 * chans
    for s in range(bands):
        row = pl.multiple_of(source_of(band, bands, s) * lats, 8)
        block = blocks[s][...] if len(blocks[s].shape) == 2 else blocks[s][field]
        fourier[pl.ds(row, lats), :] = block.astype(jnp.float32)
    for i in range(groups * per_dev):
        columns[i] = fourier[:, pl.ds(i * width, width)].astype(jnp.bfloat16)
    for q in range(groups):
        owner = jnp.bitwise_xor(group, slots[q])
        first = jnp.where(jnp.logical_and(band == 0, owner == 0), 1.0, 2.0)
        squares = None
        for o in range(per_dev):
            coef = jnp.dot(
                bases[q][o, :, :depth],
                columns[owner * per_dev + o],
                preferred_element_type=jnp.float32,
            )
            term = coef * coef * (first if o == 0 else 2.0)
            squares = term if squares is None else squares + term
        if q == 0:
            total[:, pl.ds(0, width)] = squares
        else:
            total[:, pl.ds(0, width)] += squares
    sums = total[...]
    energy = sums[:, :chans] + sums[:, chans:width]
    flat = jnp.pad(
        energy, ((0, round_up(degrees, LANES) - degrees), (0, round_up(chans, 8) - chans))
    )
    lane_tiles = round_up(degrees, LANES) // LANES
    row_tiles = round_up(chans, 8) // 8
    for k in range(lane_tiles):
        piece = flat[k * LANES : (k + 1) * LANES, :].T
        for r in range(row_tiles):
            out[r * lane_tiles + k] = piece[r * 8 : (r + 1) * 8, :]
    if field == 1:
        high = lax.rem(group, 2) == 1
        first, second = energy_before[...], out[...]
        kept[...] = jnp.where(high, second, first)
        sent[...] = jnp.where(high, first, second)


def legendre_energy(blocks, bases, slots, chans, lats, before):
    bands, groups = len(blocks), len(bases)
    per_dev, degrees, _ = bases[0].shape
    row_tiles = round_up(chans, 8) // 8
    lane_tiles = round_up(degrees, LANES) // LANES
    tiles = (row_tiles * lane_tiles, 8, LANES)
    field = len(before)
    out = jax.ShapeDtypeStruct(tiles, jnp.float32)
    return pl.pallas_call(
        functools.partial(legendre_kernel, bands, groups, per_dev, chans, lats, slots, field),
        out_shape=[out, out] if field else [out],
        scratch_shapes=([pltpu.VMEM(tiles, jnp.float32)] if field else [])
        + [
            pltpu.VMEM((bands * lats, blocks[0].shape[-1]), jnp.float32),
            pltpu.VMEM((groups * per_dev, bands * lats, 2 * chans), jnp.bfloat16),
            pltpu.VMEM((degrees, round_up(2 * chans, LANES)), jnp.float32),
        ],
        compiler_params=pltpu.CompilerParams(vmem_limit_bytes=VMEM_LIMIT),
        name="legendre",
    )(*blocks, *bases, *before)


def loss_kernel(chans, degrees, count, blocks, spectra, loss, sums):
    lane_tiles = round_up(degrees, LANES) // LANES
    row_tiles = round_up(chans, 8) // 8
    scale = 1.0 / count
    for r in range(row_tiles):
        rows = min(8, chans - r * 8)
        acc = jnp.zeros((8, LANES), jnp.float32)
        for k in range(lane_tiles):
            lanes = min(LANES, degrees - k * LANES)
            first = blocks[r * lane_tiles + k] * scale
            second = blocks[(row_tiles + r) * lane_tiles + k] * scale
            spectra[0, pl.ds(r * 8, rows), pl.ds(k * LANES, lanes)] = first[:rows, :lanes]
            spectra[1, pl.ds(r * 8, rows), pl.ds(k * LANES, lanes)] = second[:rows, :lanes]
            gap = jnp.log(first + 1e-06) - jnp.log(second + 1e-06)
            gap = gap * gap
            if lanes < LANES:
                lane_ids = lax.broadcasted_iota(jnp.int32, gap.shape, 1)
                gap = jnp.where(lane_ids < lanes, gap, 0.0)
            acc = acc + gap
        sums[pl.ds(r * 8, 8), :] = acc
    turned = sums[...].T
    loss[...] = (jnp.sum(turned, axis=0, keepdims=True) * (1.0 / degrees))[:, :chans]


def loss_call(blocks, chans, degrees, count):
    return pl.pallas_call(
        functools.partial(loss_kernel, chans, degrees, count),
        out_shape=(
            jax.ShapeDtypeStruct((2, chans, degrees), jnp.float32),
            jax.ShapeDtypeStruct((1, chans), jnp.float32),
        ),
        scratch_shapes=[pltpu.VMEM((round_up(chans, 8), LANES), jnp.float32)],
        compiler_params=pltpu.CompilerParams(vmem_limit_bytes=VMEM_LIMIT),
        name="loss",
    )(blocks)


def exchange(value, axis, step):
    return lax.ppermute(value, axis, peers(lax.axis_size(axis), step))


def reduce_all(kept, sent):
    index = lax.axis_index("batch")
    groups = lax.axis_size("batch")
    value = kept + exchange(sent, "batch", 1)
    halved = [(1, index % 2 == 1)]
    step = 2
    while step < groups:
        if value.shape[0] % 2 == 0:
            half = value.shape[0] // 2
            high = (index // step) % 2 == 1
            lower, upper = value[:half], value[half:]
            kept = jnp.where(high, upper, lower)
            sent = jnp.where(high, lower, upper)
            value = kept + exchange(sent, "batch", step)
            halved.append((step, high))
        else:
            value = value + exchange(value, "batch", step)
        step *= 2
    bands = lax.axis_size("lat")
    step = 1
    radix = 2 if bands.bit_length() % 2 == 0 else 4
    while step < bands:
        parts = [exchange(value, "lat", k * step) for k in range(radix - 1, 0, -1)]
        value = value + sum(parts[1:], parts[0])
        step *= radix
        radix = 4
    for step, high in reversed(halved):
        other = exchange(value, "batch", step)
        value = jnp.where(
            high, jnp.concatenate([other, value]), jnp.concatenate([value, other])
        )
    return value


def spectrum_loss(predicted, target, legendre_basis):
    groups = lax.axis_size("batch")
    bands = lax.axis_size("lat")
    per_dev = legendre_basis.shape[1]
    members, chans, lats, lon_count = predicted.shape
    degrees = legendre_basis.shape[2]
    table = jnp.asarray(fourier_table(lon_count, groups, bands, per_dev))
    rows = members * chans * lats
    far, near = reach(bands)
    basis = jnp.transpose(legendre_basis, (1, 0, 2))
    bases, slots = [basis], [0]
    step = groups // 2
    while step:
        bases = bases + [exchange(block, "batch", step) for block in bases]
        slots = slots + [slot ^ step for slot in slots]
        step //= 2

    def transform(field, before):
        flat = field.reshape(rows, lon_count)
        return dft_blocks(flat, table, before, bands, groups * per_dev * 2, chans, lats)

    first = transform(predicted, [])
    second = transform(target, [first[s] for s in sorted(near)])
    got0, got1 = {0: first[0]}, {0: second[0]}
    for s in far:
        got0[s] = exchange(first[s], "lat", s)
        got1[s] = exchange(second[s], "lat", s)
    for s in near:
        got0[s] = got1[s] = exchange(second[s], "lat", s)
    bases = turned_bases(bases)
    blocks = [got0[s] for s in range(bands)]
    before = legendre_energy(blocks, bases, slots, chans, lats, [])
    blocks = [got1[s] for s in range(bands)]
    kept, sent = legendre_energy(blocks, bases, slots, chans, lats, before)
    energy = reduce_all(kept, sent)
    spectra, loss = loss_call(
        energy, chans, degrees, members * groups * groups * bands * per_dev
    )
    return (spectra, loss.reshape(chans))


def reach(bands):
    steps = range(bands - 1, 0, -1)
    return [s for s in steps if s >= bands // 2], [s for s in steps if s < bands // 2]


def solution(mesh):
    placed = (
        P("batch", None, "lat", None),
        P("batch", None, "lat", None),
        P(None, ("batch", "lat"), None),
    )
    return jax.shard_map(spectrum_loss, mesh=mesh, in_specs=placed, out_specs=(P(), P()), check_vma=False)
```

```python
import functools
import math

import jax
import jax.numpy as jnp
import numpy as np
from jax import lax
from jax.experimental import pallas as pl
from jax.experimental.pallas import tpu as pltpu
from jax.sharding import PartitionSpec as P


LANES = 128
VMEM_LIMIT = 24 * 1024 * 1024
STAGED_LIMIT = 53 * 1024 * 1024
DIRECT_LIMIT = 44 * 1024 * 1024


def round_up(value, step):
    return -(-value // step) * step


def fourier_table(lon_count, groups, bands, per_dev):
    orders = np.arange(groups * bands * per_dev).reshape(groups, bands, per_dev)
    orders = orders.transpose(1, 0, 2).reshape(-1)
    product_ids = np.arange(lon_count)[:, None] * orders[None, :] % lon_count
    angles = np.float32(2.0 * math.pi / lon_count) * product_ids.astype(np.float32)
    inv_root = np.float32(1.0 / math.sqrt(lon_count))
    both = np.stack([np.cos(angles) * inv_root, -np.sin(angles) * inv_root], axis=2)
    flat = both.reshape(lon_count, -1).astype(jnp.bfloat16)
    padded = round_up(flat.shape[1], LANES)
    return np.pad(flat, ((0, 0), (0, padded - flat.shape[1])))


def peers(count, step):
    if count & (count - 1) == 0:
        return [(i, i ^ step) for i in range(count)]
    return [(i, (i + step) % count) for i in range(count)]


def target_of(index, count, step):
    if count & (count - 1) == 0:
        return jnp.bitwise_xor(index, step)
    return lax.rem(index + step, count)


def source_of(index, count, step):
    if count & (count - 1) == 0:
        return jnp.bitwise_xor(index, step)
    return lax.rem(index + count - step, count)


def dft_kernel(bands, per, chans, lats, chunks, field, table_hbm, *rest):
    outs = rest[:bands]
    dscr, turned, packed = rest[bands : bands + 3]
    staged = len(rest) > bands + 3
    if staged:
        xbuf, table, sems = rest[bands + 3 :]
        load = pltpu.make_async_copy(table_hbm, table, sems.at[len(chunks)])
        load.start()
    else:
        xbuf, table = field, table_hbm
    copies = []
    row = 0
    for i, rows in enumerate(chunks):
        cp = None
        if staged:
            cp = pltpu.make_async_copy(
                field.at[pl.ds(row, rows), :], xbuf.at[pl.ds(row, rows), :], sems.at[i]
            )
            cp.start()
        copies.append((row, rows, cp))
        row += rows
    band = lax.axis_index("lat")
    tiles = dscr.shape[0]
    if staged:
        load.wait()
    for row, rows, cp in copies:
        if staged:
            cp.wait()
        res = jnp.dot(xbuf[pl.ds(row, rows), :], table[...], preferred_element_type=jnp.float32)
        for q in range(tiles):
            dscr[q, pl.ds(row, rows), :] = res[:, q * LANES : (q + 1) * LANES]

    def turn(q, carry):
        for n in range(lats):
            block = dscr.at[q][pl.ds(n, LANES, stride=lats), :]
            turned.at[q][pl.ds(n, LANES, stride=lats), :] = block.T
        return carry

    lax.fori_loop(0, tiles, turn, 0)

    def pack(s, carry):
        base = target_of(band, bands, s) * per
        for g in range(per):
            column = base + g
            start = pl.multiple_of(lax.rem(column, LANES) * lats, 8)
            packed[s, :, pl.ds(g * chans, chans)] = turned[
                column // LANES, pl.ds(start, lats), pl.ds(0, chans)
            ]
        return carry

    lax.fori_loop(0, bands, pack, 0, unroll=min(bands, 8))
    for s in range(bands):
        outs[s][...] = packed[s].astype(jnp.bfloat16)


def dft_blocks(field, table, staged, bands, per, chans, lats):
    rows_all, lon_count = field.shape
    width = round_up(per * chans, LANES)
    step = -(-chans // 3) * lats
    chunks = []
    left = rows_all
    while left > 0:
        chunks.append(min(step, left))
        left -= step
    columns = table.shape[1]
    anywhere = pl.BlockSpec(memory_space=pl.ANY)
    vmem = pl.BlockSpec(memory_space=pltpu.VMEM)
    staging = [
        pltpu.VMEM((rows_all, lon_count), jnp.bfloat16),
        pltpu.VMEM(table.shape, jnp.bfloat16),
        pltpu.SemaphoreType.DMA((len(chunks) + 1,)),
    ]
    staging = staging if staged else []
    return pl.pallas_call(
        functools.partial(dft_kernel, bands, per, chans, lats, tuple(chunks)),
        out_shape=[jax.ShapeDtypeStruct((lats, width), jnp.bfloat16)] * bands,
        in_specs=[anywhere if staged else vmem] * 2,
        out_specs=[vmem] * bands,
        scratch_shapes=[
            pltpu.VMEM((columns // LANES, LANES * lats, LANES), jnp.float32),
            pltpu.VMEM((columns // LANES, LANES * lats, LANES), jnp.float32),
            pltpu.VMEM((bands, lats, width), jnp.float32),
        ]
        + staging,
        compiler_params=pltpu.CompilerParams(
            vmem_limit_bytes=STAGED_LIMIT if staged else DIRECT_LIMIT
        ),
        name="dft",
    )(field, table)


def turn_kernel(count, *refs):
    for basis, out in zip(refs[:count], refs[count:]):
        for o in range(basis.shape[0]):
            out[o, :, : basis.shape[1]] = basis[o].T


def turned_bases(bases):
    per_dev, lat_count, degrees = bases[0].shape
    shape = (per_dev, degrees, round_up(lat_count, LANES))
    return pl.pallas_call(
        functools.partial(turn_kernel, len(bases)),
        out_shape=[jax.ShapeDtypeStruct(shape, bases[0].dtype)] * len(bases),
        compiler_params=pltpu.CompilerParams(vmem_limit_bytes=VMEM_LIMIT),
        name="turn",
    )(*bases)


def legendre_kernel(bands, groups, per_dev, chans, lats, slots, field, *rest):
    blocks = rest[:bands]
    bases = rest[bands : bands + groups]
    rest = rest[bands + groups :]
    fourier, columns, total = rest[-3:]
    if field == 0:
        out = rest[0]
    else:
        energy_before, kept, sent, out = rest[0], rest[1], rest[2], rest[3]
    band, group = lax.axis_index("lat"), lax.axis_index("batch")
    degrees = bases[0].shape[1]
    depth = bands * lats
    width = 2 * chans
    for s in range(bands):
        row = pl.multiple_of(source_of(band, bands, s) * lats, 8)
        fourier[pl.ds(row, lats), :] = blocks[s][...].astype(jnp.float32)
    for i in range(groups * per_dev):
        columns[i] = fourier[:, pl.ds(i * width, width)].astype(jnp.bfloat16)
    for q in range(groups):
        owner = jnp.bitwise_xor(group, slots[q])
        first = jnp.where(jnp.logical_and(band == 0, owner == 0), 1.0, 2.0)
        squares = None
        for o in range(per_dev):
            coef = jnp.dot(
                bases[q][o, :, :depth],
                columns[owner * per_dev + o],
                preferred_element_type=jnp.float32,
            )
            term = coef * coef * (first if o == 0 else 2.0)
            squares = term if squares is None else squares + term
        if q == 0:
            total[:, pl.ds(0, width)] = squares
        else:
            total[:, pl.ds(0, width)] += squares
    sums = total[...]
    energy = sums[:, :chans] + sums[:, chans:width]
    flat = jnp.pad(
        energy, ((0, round_up(degrees, LANES) - degrees), (0, round_up(chans, 8) - chans))
    )
    lane_tiles = round_up(degrees, LANES) // LANES
    row_tiles = round_up(chans, 8) // 8
    for k in range(lane_tiles):
        piece = flat[k * LANES : (k + 1) * LANES, :].T
        for r in range(row_tiles):
            out[r * lane_tiles + k] = piece[r * 8 : (r + 1) * 8, :]
    if field == 1:
        high = lax.rem(group, 2) == 1
        first, second = energy_before[...], out[...]
        kept[...] = jnp.where(high, second, first)
        sent[...] = jnp.where(high, first, second)


def legendre_energy(blocks, bases, slots, chans, lats, before):
    bands, groups = len(blocks), len(bases)
    per_dev, degrees, _ = bases[0].shape
    row_tiles = round_up(chans, 8) // 8
    lane_tiles = round_up(degrees, LANES) // LANES
    tiles = (row_tiles * lane_tiles, 8, LANES)
    field = len(before)
    out = jax.ShapeDtypeStruct(tiles, jnp.float32)
    return pl.pallas_call(
        functools.partial(legendre_kernel, bands, groups, per_dev, chans, lats, slots, field),
        out_shape=[out, out] if field else [out],
        scratch_shapes=([pltpu.VMEM(tiles, jnp.float32)] if field else [])
        + [
            pltpu.VMEM((bands * lats, blocks[0].shape[-1]), jnp.float32),
            pltpu.VMEM((groups * per_dev, bands * lats, 2 * chans), jnp.bfloat16),
            pltpu.VMEM((degrees, round_up(2 * chans, LANES)), jnp.float32),
        ],
        compiler_params=pltpu.CompilerParams(vmem_limit_bytes=VMEM_LIMIT),
        name="legendre",
    )(*blocks, *bases, *before)


def loss_kernel(chans, degrees, count, mesh_size, *refs):
    parts = (len(refs) - 4) // 2
    owned, other = refs[:parts], refs[parts : 2 * parts]
    spectra, loss, sums, fields = refs[2 * parts :]
    lane_tiles = round_up(degrees, LANES) // LANES
    row_tiles = round_up(chans, 8) // 8
    scale = 1.0 / count
    mine = quarter_id(mesh_size)
    high = lax.rem(lax.axis_index("batch"), 2)
    size = owned[0].shape[0]
    for m in range(parts):
        start = jnp.bitwise_xor(mine, m) * size
        fields[high, pl.ds(start, size)] = owned[m][...] * scale
        fields[1 - high, pl.ds(start, size)] = other[m][...] * scale
    for r in range(row_tiles):
        rows = min(8, chans - r * 8)
        acc = jnp.zeros((8, LANES), jnp.float32)
        for k in range(lane_tiles):
            lanes = min(LANES, degrees - k * LANES)
            first = fields[0, r * lane_tiles + k]
            second = fields[1, r * lane_tiles + k]
            spectra[0, pl.ds(r * 8, rows), pl.ds(k * LANES, lanes)] = first[:rows, :lanes]
            spectra[1, pl.ds(r * 8, rows), pl.ds(k * LANES, lanes)] = second[:rows, :lanes]
            gap = jnp.log(first + 1e-06) - jnp.log(second + 1e-06)
            gap = gap * gap
            if lanes < LANES:
                lane_ids = lax.broadcasted_iota(jnp.int32, gap.shape, 1)
                gap = jnp.where(lane_ids < lanes, gap, 0.0)
            acc = acc + gap
        sums[pl.ds(r * 8, 8), :] = acc
    turned = sums[...].T
    loss[...] = (jnp.sum(turned, axis=0, keepdims=True) * (1.0 / degrees))[:, :chans]


def loss_call(owned, other, chans, degrees, count):
    mesh_size = lax.axis_size("batch"), lax.axis_size("lat")
    tiles = len(owned) * owned[0].shape[0]
    return pl.pallas_call(
        functools.partial(loss_kernel, chans, degrees, count, mesh_size),
        out_shape=(
            jax.ShapeDtypeStruct((2, chans, degrees), jnp.float32),
            jax.ShapeDtypeStruct((1, chans), jnp.float32),
        ),
        scratch_shapes=[
            pltpu.VMEM((round_up(chans, 8), LANES), jnp.float32),
            pltpu.VMEM((2, tiles, 8, LANES), jnp.float32),
        ],
        compiler_params=pltpu.CompilerParams(vmem_limit_bytes=VMEM_LIMIT),
        name="loss",
    )(*owned, *other)


def exchange(value, axis, step):
    return lax.ppermute(value, axis, peers(lax.axis_size(axis), step))


def square(mesh_size):
    groups, bands = mesh_size
    return [bit for bit, there in ((1, bands > 1), (2 * bands, groups > 2)) if there]


def quarter_steps(mesh_size):
    bits = square(mesh_size)
    return [sum(bit for k, bit in enumerate(bits) if m >> k & 1) for m in range(1 << len(bits))]


def quarter_id(mesh_size):
    _, bands = mesh_size
    flat = lax.axis_index("batch") * bands + lax.axis_index("lat")
    return sum(lax.rem(flat // bit, 2) << k for k, bit in enumerate(square(mesh_size)))


def flat_exchange(value, mesh_size, step):
    count = mesh_size[0] * mesh_size[1]
    return lax.ppermute(value, ("batch", "lat"), [(i, i ^ step) for i in range(count)])


def reduce_all(kept, sent):
    mesh_size = groups, bands = lax.axis_size("batch"), lax.axis_size("lat")
    value = kept + exchange(sent, "batch", 1)
    steps = quarter_steps(mesh_size)
    mine = quarter_id(mesh_size)
    pieces = value.reshape((len(steps), value.shape[0] // len(steps)) + value.shape[1:])
    value = lax.dynamic_index_in_dim(pieces, mine, 0, keepdims=False)
    for m in range(len(steps) - 1, 0, -1):
        piece = lax.dynamic_index_in_dim(pieces, jnp.bitwise_xor(mine, m), 0, keepdims=False)
        value = value + flat_exchange(piece, mesh_size, steps[m])
    step = 4
    while step < groups:
        value = value + exchange(value, "batch", step)
        step *= 2
    step = 2
    radix = 2 if bands.bit_length() % 2 == 1 else 4
    while step < bands:
        parts = [exchange(value, "lat", k * step) for k in range(radix - 1, 0, -1)]
        value = value + sum(parts[1:], parts[0])
        step *= radix
        radix = 4
    owned = [flat_exchange(value, mesh_size, step) if step else value for step in steps]
    return owned, [exchange(piece, "batch", 1) for piece in owned]


def spectrum_loss(predicted, target, legendre_basis):
    groups = lax.axis_size("batch")
    bands = lax.axis_size("lat")
    per_dev = legendre_basis.shape[1]
    members, chans, lats, lon_count = predicted.shape
    degrees = legendre_basis.shape[2]
    table = jnp.asarray(fourier_table(lon_count, groups, bands, per_dev))
    rows = members * chans * lats
    far, near = reach(bands)
    basis = jnp.transpose(legendre_basis, (1, 0, 2))
    bases, slots = [basis], [0]
    step = groups // 2
    while step:
        bases = bases + [exchange(block, "batch", step) for block in bases]
        slots = slots + [slot ^ step for slot in slots]
        step //= 2

    def transform(field, staged):
        flat = field.reshape(rows, lon_count)
        return dft_blocks(flat, table, staged, bands, groups * per_dev * 2, chans, lats)

    first = transform(predicted, True)
    second = transform(target, False)
    got0, got1 = {0: first[0]}, {0: second[0]}
    for s in far + near:
        got0[s] = exchange(first[s], "lat", s)
        got1[s] = exchange(second[s], "lat", s)
    bases = turned_bases(bases)
    blocks = [got0[s] for s in range(bands)]
    before = legendre_energy(blocks, bases, slots, chans, lats, [])
    blocks = [got1[s] for s in range(bands)]
    kept, sent = legendre_energy(blocks, bases, slots, chans, lats, before)
    owned, other = reduce_all(kept, sent)
    spectra, loss = loss_call(
        owned, other, chans, degrees, members * groups * groups * bands * per_dev
    )
    return (spectra, loss.reshape(chans))


def reach(bands):
    steps = range(bands - 1, 0, -1)
    return [s for s in steps if s >= bands // 2], [s for s in steps if s < bands // 2]


def solution(mesh):
    placed = (
        P("batch", None, "lat", None),
        P("batch", None, "lat", None),
        P(None, ("batch", "lat"), None),
    )
    return jax.shard_map(spectrum_loss, mesh=mesh, in_specs=placed, out_specs=(P(), P()), check_vma=False)
```

```python
import functools
import math

import jax
import jax.numpy as jnp
import numpy as np
from jax import lax
from jax.experimental import pallas as pl
from jax.experimental.pallas import tpu as pltpu
from jax.sharding import PartitionSpec as P


LANES = 128
SPARE_VMEM = 16 * 1024 * 1024
VMEM_LIMIT = 24 * 1024 * 1024
STAGED_LIMIT = 53 * 1024 * 1024
DIRECT_LIMIT = 44 * 1024 * 1024


def round_up(value, step):
    return -(-value // step) * step


def fourier_table(lon_count, groups, bands, per_dev):
    orders = np.arange(groups * bands * per_dev).reshape(groups, bands, per_dev)
    orders = orders.transpose(1, 0, 2).reshape(-1)
    product_ids = np.arange(lon_count)[:, None] * orders[None, :] % lon_count
    angles = np.float32(2.0 * math.pi / lon_count) * product_ids.astype(np.float32)
    inv_root = np.float32(1.0 / math.sqrt(lon_count))
    both = np.stack([np.cos(angles) * inv_root, -np.sin(angles) * inv_root], axis=2)
    flat = both.reshape(lon_count, -1).astype(jnp.bfloat16)
    padded = round_up(flat.shape[1], LANES)
    return np.pad(flat, ((0, 0), (0, padded - flat.shape[1])))


def peers(count, step):
    if count & (count - 1) == 0:
        return [(i, i ^ step) for i in range(count)]
    return [(i, (i + step) % count) for i in range(count)]


def target_of(index, count, step):
    if count & (count - 1) == 0:
        return jnp.bitwise_xor(index, step)
    return lax.rem(index + step, count)


def source_of(index, count, step):
    if count & (count - 1) == 0:
        return jnp.bitwise_xor(index, step)
    return lax.rem(index + count - step, count)


def dft_kernel(bands, per, chans, lats, chunks, field, table_hbm, *rest):
    outs = rest[:bands]
    dscr, turned, packed = rest[bands : bands + 3]
    staged = len(rest) > bands + 3
    if staged:
        xbuf, table, sems = rest[bands + 3 :]
        load = pltpu.make_async_copy(table_hbm, table, sems.at[len(chunks)])
        load.start()
    else:
        xbuf, table = field, table_hbm
    copies = []
    row = 0
    for i, rows in enumerate(chunks):
        cp = None
        if staged:
            cp = pltpu.make_async_copy(
                field.at[pl.ds(row, rows), :], xbuf.at[pl.ds(row, rows), :], sems.at[i]
            )
            cp.start()
        copies.append((row, rows, cp))
        row += rows
    band = lax.axis_index("lat")
    tiles = dscr.shape[0]
    if staged:
        load.wait()
    for row, rows, cp in copies:
        if staged:
            cp.wait()
        res = jnp.dot(xbuf[pl.ds(row, rows), :], table[...], preferred_element_type=jnp.float32)
        for q in range(tiles):
            dscr[q, pl.ds(row, rows), :] = res[:, q * LANES : (q + 1) * LANES]

    def turn(q, carry):
        for n in range(lats):
            block = dscr.at[q][pl.ds(n, LANES, stride=lats), :]
            turned.at[q][pl.ds(n, LANES, stride=lats), :] = block.T
        return carry

    lax.fori_loop(0, tiles, turn, 0)

    def pack(s, carry):
        base = target_of(band, bands, s) * per
        for g in range(per):
            column = base + g
            start = pl.multiple_of(lax.rem(column, LANES) * lats, 8)
            packed[s, :, pl.ds(g * chans, chans)] = turned[
                column // LANES, pl.ds(start, lats), pl.ds(0, chans)
            ]
        return carry

    lax.fori_loop(0, bands, pack, 0, unroll=min(bands, 8))
    for s in range(bands):
        outs[s][...] = packed[s].astype(jnp.bfloat16)


def rows_kernel(bands, per, chunks, field, table_hbm, *rest):
    outs = rest[:bands]
    dscr, turned, xbuf, table, sems = rest[bands:]
    load = pltpu.make_async_copy(table_hbm, table, sems.at[len(chunks)])
    load.start()
    copies = []
    row = 0
    for i, rows in enumerate(chunks):
        cp = pltpu.make_async_copy(
            field.at[pl.ds(row, rows), :], xbuf.at[pl.ds(row, rows), :], sems.at[i]
        )
        cp.start()
        copies.append((row, rows, cp))
        row += rows
    load.wait()
    tiles = dscr.shape[0]
    for row, rows, cp in copies:
        cp.wait()
        res = jnp.dot(xbuf[pl.ds(row, rows), :], table[...], preferred_element_type=jnp.float32)
        for q in range(tiles):
            dscr[q, pl.ds(row, rows), :] = res[:, q * LANES : (q + 1) * LANES]
            for start in range(row, row + rows, LANES):
                block = dscr[q, pl.ds(start, LANES), :]
                turned[pl.ds(q * LANES, LANES), pl.ds(start, LANES)] = block.T
    band = lax.axis_index("lat")
    for s in range(bands):
        start = pl.multiple_of(target_of(band, bands, s) * per, 8)
        outs[s][...] = turned[pl.ds(start, per), :].astype(jnp.bfloat16)


def row_blocks(field, table, bands, per):
    rows_all, lon_count = field.shape
    width = round_up(rows_all, LANES)
    columns = table.shape[1]
    step = 4 * LANES
    chunks = [min(step, rows_all - row) for row in range(0, rows_all, step)]
    anywhere = pl.BlockSpec(memory_space=pl.ANY)
    vmem = pl.BlockSpec(memory_space=pltpu.VMEM)
    return pl.pallas_call(
        functools.partial(rows_kernel, bands, per, tuple(chunks)),
        out_shape=[jax.ShapeDtypeStruct((per, width), jnp.bfloat16)] * bands,
        in_specs=[anywhere] * 2,
        out_specs=[vmem] * bands,
        scratch_shapes=[
            pltpu.VMEM((columns // LANES, width, LANES), jnp.float32),
            pltpu.VMEM((columns, width), jnp.float32),
            pltpu.VMEM((rows_all, lon_count), jnp.bfloat16),
            pltpu.VMEM(table.shape, jnp.bfloat16),
            pltpu.SemaphoreType.DMA((len(chunks) + 1,)),
        ],
        compiler_params=pltpu.CompilerParams(vmem_limit_bytes=STAGED_LIMIT),
        name="dft_rows",
    )(field, table)


def dft_blocks(field, table, staged, bands, per, chans, lats):
    rows_all, lon_count = field.shape
    width = round_up(per * chans, LANES)
    step = -(-chans // 3) * lats
    chunks = []
    left = rows_all
    while left > 0:
        chunks.append(min(step, left))
        left -= step
    columns = table.shape[1]
    anywhere = pl.BlockSpec(memory_space=pl.ANY)
    vmem = pl.BlockSpec(memory_space=pltpu.VMEM)
    staging = [
        pltpu.VMEM((rows_all, lon_count), jnp.bfloat16),
        pltpu.VMEM(table.shape, jnp.bfloat16),
        pltpu.SemaphoreType.DMA((len(chunks) + 1,)),
    ]
    staging = staging if staged else []
    return pl.pallas_call(
        functools.partial(dft_kernel, bands, per, chans, lats, tuple(chunks)),
        out_shape=[jax.ShapeDtypeStruct((lats, width), jnp.bfloat16)] * bands,
        in_specs=[anywhere if staged else vmem] * 2,
        out_specs=[vmem] * bands,
        scratch_shapes=[
            pltpu.VMEM((columns // LANES, LANES * lats, LANES), jnp.float32),
            pltpu.VMEM((columns // LANES, LANES * lats, LANES), jnp.float32),
            pltpu.VMEM((bands, lats, width), jnp.float32),
        ]
        + staging,
        compiler_params=pltpu.CompilerParams(
            vmem_limit_bytes=STAGED_LIMIT if staged else DIRECT_LIMIT
        ),
        name="dft",
    )(field, table)


def turn_kernel(count, *refs):
    for basis, out in zip(refs[:count], refs[count:]):
        for o in range(basis.shape[0]):
            out[o, :, : basis.shape[1]] = basis[o].T


def turned_bases(bases):
    per_dev, lat_count, degrees = bases[0].shape
    shape = (per_dev, degrees, round_up(lat_count, LANES))
    return pl.pallas_call(
        functools.partial(turn_kernel, len(bases)),
        out_shape=[jax.ShapeDtypeStruct(shape, bases[0].dtype)] * len(bases),
        compiler_params=pltpu.CompilerParams(vmem_limit_bytes=VMEM_LIMIT),
        name="turn",
    )(*bases)


def prepare_kernel(bands, lats, chans, *refs):
    blocks, (columns, rows, flat, planes) = refs[:bands], refs[bands:]
    band = lax.axis_index("lat")
    per, width = blocks[0].shape
    fit = LANES // per
    depth = bands * lats
    for s in range(bands):
        source = source_of(band, bands, s)
        start = pl.multiple_of(source // fit * LANES + lax.rem(source, fit) * per, 8)
        rows[pl.ds(start, per), :] = blocks[s][...].astype(jnp.float32)
    tiles = flat.shape[0]
    for q in range(tiles):
        for start in range(0, width, LANES):
            block = rows[pl.ds(q * LANES, LANES), pl.ds(start, LANES)]
            flat[q, pl.ds(start, LANES), :] = block.T
    for q in range(tiles):
        for n in range(lats):
            block = flat.at[q][pl.ds(n, round_up(chans, 8), stride=lats), :].T
            for k in range(min(fit, bands - q * fit)):
                place = pl.ds((q * fit + k) * lats + n, per, stride=depth)
                planes[place, :] = jnp.pad(
                    block[k * per : (k + 1) * per, :], ((0, 0), (0, LANES - block.shape[1]))
                )
    for i in range(per // 2):
        for p in range(2):
            piece = planes[pl.ds((2 * i + p) * depth, depth), pl.ds(0, chans)]
            columns[i, :, pl.ds(p * chans, chans)] = piece.astype(jnp.bfloat16)


def prepared_columns(blocks, lats, chans):
    bands = len(blocks)
    per, width = blocks[0].shape
    tiles = -(-bands // (LANES // per))
    shape = (per // 2, bands * lats, 2 * chans)
    held = 4 * LANES * (tiles * (width + LANES * lats) + per * bands * lats)
    return pl.pallas_call(
        functools.partial(prepare_kernel, bands, lats, chans),
        out_shape=jax.ShapeDtypeStruct(shape, jnp.bfloat16),
        scratch_shapes=[
            pltpu.VMEM((tiles * LANES, width), jnp.float32),
            pltpu.VMEM((tiles, LANES * lats, LANES), jnp.float32),
            pltpu.VMEM((per * bands * lats, LANES), jnp.float32),
        ],
        compiler_params=pltpu.CompilerParams(vmem_limit_bytes=SPARE_VMEM + held),
        name="prepare",
    )(*blocks)


def legendre_kernel(bands, groups, per_dev, chans, lats, slots, field, *rest):
    inputs = bands if field else 1
    blocks = rest[:inputs]
    bases = rest[inputs : inputs + groups]
    rest = rest[inputs + groups :]
    total = rest[-1]
    if field == 0:
        out, columns = rest[0], blocks[0]
    else:
        energy_before, kept, sent, out, fourier, columns = rest[:6]
    band, group = lax.axis_index("lat"), lax.axis_index("batch")
    degrees = bases[0].shape[1]
    depth = bands * lats
    width = 2 * chans
    if field:
        for s in range(bands):
            row = pl.multiple_of(source_of(band, bands, s) * lats, 8)
            fourier[pl.ds(row, lats), :] = blocks[s][...].astype(jnp.float32)
        for i in range(groups * per_dev):
            columns[i] = fourier[:, pl.ds(i * width, width)].astype(jnp.bfloat16)
    for q in range(groups):
        owner = jnp.bitwise_xor(group, slots[q])
        first = jnp.where(jnp.logical_and(band == 0, owner == 0), 1.0, 2.0)
        squares = None
        for o in range(per_dev):
            coef = jnp.dot(
                bases[q][o, :, :depth],
                columns[owner * per_dev + o],
                preferred_element_type=jnp.float32,
            )
            term = coef * coef * (first if o == 0 else 2.0)
            squares = term if squares is None else squares + term
        if q == 0:
            total[:, pl.ds(0, width)] = squares
        else:
            total[:, pl.ds(0, width)] += squares
    sums = total[...]
    energy = sums[:, :chans] + sums[:, chans:width]
    flat = jnp.pad(
        energy, ((0, round_up(degrees, LANES) - degrees), (0, round_up(chans, 8) - chans))
    )
    lane_tiles = round_up(degrees, LANES) // LANES
    row_tiles = round_up(chans, 8) // 8
    for k in range(lane_tiles):
        piece = flat[k * LANES : (k + 1) * LANES, :].T
        for r in range(row_tiles):
            out[r * lane_tiles + k] = piece[r * 8 : (r + 1) * 8, :]
    if field == 1:
        high = lax.rem(group, 2) == 1
        first, second = energy_before[...], out[...]
        kept[...] = jnp.where(high, second, first)
        sent[...] = jnp.where(high, first, second)


def legendre_energy(blocks, bases, slots, chans, lats, bands, before):
    groups = len(bases)
    per_dev, degrees, _ = bases[0].shape
    row_tiles = round_up(chans, 8) // 8
    lane_tiles = round_up(degrees, LANES) // LANES
    tiles = (row_tiles * lane_tiles, 8, LANES)
    field = len(before)
    out = jax.ShapeDtypeStruct(tiles, jnp.float32)
    staging = [
        pltpu.VMEM(tiles, jnp.float32),
        pltpu.VMEM((bands * lats, blocks[0].shape[-1]), jnp.float32),
        pltpu.VMEM((groups * per_dev, bands * lats, 2 * chans), jnp.bfloat16),
    ]
    return pl.pallas_call(
        functools.partial(legendre_kernel, bands, groups, per_dev, chans, lats, slots, field),
        out_shape=[out, out] if field else [out],
        scratch_shapes=(staging if field else [])
        + [pltpu.VMEM((degrees, round_up(2 * chans, LANES)), jnp.float32)],
        compiler_params=pltpu.CompilerParams(vmem_limit_bytes=VMEM_LIMIT),
        name="legendre",
    )(*blocks, *bases, *before)


def loss_kernel(chans, degrees, count, mesh_size, *refs):
    parts = (len(refs) - 4) // 2
    owned, other = refs[:parts], refs[parts : 2 * parts]
    spectra, loss, sums, fields = refs[2 * parts :]
    lane_tiles = round_up(degrees, LANES) // LANES
    row_tiles = round_up(chans, 8) // 8
    scale = 1.0 / count
    mine = quarter_id(mesh_size)
    high = lax.rem(lax.axis_index("batch"), 2)
    size = owned[0].shape[0]
    for m in range(parts):
        start = jnp.bitwise_xor(mine, m) * size
        fields[high, pl.ds(start, size)] = owned[m][...] * scale
        fields[1 - high, pl.ds(start, size)] = other[m][...] * scale
    for r in range(row_tiles):
        rows = min(8, chans - r * 8)
        acc = jnp.zeros((8, LANES), jnp.float32)
        for k in range(lane_tiles):
            lanes = min(LANES, degrees - k * LANES)
            first = fields[0, r * lane_tiles + k]
            second = fields[1, r * lane_tiles + k]
            spectra[pl.ds(r * 8, rows), 0, pl.ds(k * LANES, lanes)] = first[:rows, :lanes]
            spectra[pl.ds(r * 8, rows), 1, pl.ds(k * LANES, lanes)] = second[:rows, :lanes]
            gap = jnp.log(first + 1e-06) - jnp.log(second + 1e-06)
            gap = gap * gap
            if lanes < LANES:
                lane_ids = lax.broadcasted_iota(jnp.int32, gap.shape, 1)
                gap = jnp.where(lane_ids < lanes, gap, 0.0)
            acc = acc + gap
        sums[pl.ds(r * 8, 8), :] = acc
    turned = sums[...].T
    loss[...] = (jnp.sum(turned, axis=0, keepdims=True) * (1.0 / degrees))[:, :chans]


def loss_call(owned, other, chans, degrees, count):
    mesh_size = lax.axis_size("batch"), lax.axis_size("lat")
    tiles = len(owned) * owned[0].shape[0]
    return pl.pallas_call(
        functools.partial(loss_kernel, chans, degrees, count, mesh_size),
        out_shape=(
            jax.ShapeDtypeStruct((chans, 2, degrees), jnp.float32),
            jax.ShapeDtypeStruct((1, chans), jnp.float32),
        ),
        scratch_shapes=[
            pltpu.VMEM((round_up(chans, 8), LANES), jnp.float32),
            pltpu.VMEM((2, tiles, 8, LANES), jnp.float32),
        ],
        compiler_params=pltpu.CompilerParams(vmem_limit_bytes=VMEM_LIMIT),
        name="loss",
    )(*owned, *other)


def exchange(value, axis, step):
    return lax.ppermute(value, axis, peers(lax.axis_size(axis), step))


def square(mesh_size):
    groups, bands = mesh_size
    return [bit for bit, there in ((1, bands > 1), (2 * bands, groups > 2)) if there]


def quarter_steps(mesh_size):
    bits = square(mesh_size)
    return [sum(bit for k, bit in enumerate(bits) if m >> k & 1) for m in range(1 << len(bits))]


def quarter_id(mesh_size):
    _, bands = mesh_size
    flat = lax.axis_index("batch") * bands + lax.axis_index("lat")
    return sum(lax.rem(flat // bit, 2) << k for k, bit in enumerate(square(mesh_size)))


def flat_exchange(value, mesh_size, step):
    count = mesh_size[0] * mesh_size[1]
    return lax.ppermute(value, ("batch", "lat"), [(i, i ^ step) for i in range(count)])


def reduce_all(kept, sent):
    mesh_size = groups, bands = lax.axis_size("batch"), lax.axis_size("lat")
    value = kept + exchange(sent, "batch", 1)
    steps = quarter_steps(mesh_size)
    mine = quarter_id(mesh_size)
    pieces = value.reshape((len(steps), value.shape[0] // len(steps)) + value.shape[1:])
    value = lax.dynamic_index_in_dim(pieces, mine, 0, keepdims=False)
    for m in range(len(steps) - 1, 0, -1):
        piece = lax.dynamic_index_in_dim(pieces, jnp.bitwise_xor(mine, m), 0, keepdims=False)
        piece = flat_exchange(piece, mesh_size, steps[m])
        value = value + piece
    step = 4
    while step < groups:
        value = value + exchange(value, "batch", step)
        step *= 2
    step = 2
    radix = 2 if bands.bit_length() % 2 == 1 else 4
    while step < bands:
        parts = [exchange(value, "lat", k * step) for k in range(radix - 1, 0, -1)]
        value = value + sum(parts[1:], parts[0])
        step *= radix
        radix = 4
    owned = [value]
    for m in range(1, len(steps)):
        owned.append(flat_exchange(value, mesh_size, steps[m]))
    return owned, [exchange(piece, "batch", 1) for piece in owned]


def spectrum_loss(predicted, target, legendre_basis):
    groups = lax.axis_size("batch")
    bands = lax.axis_size("lat")
    per_dev = legendre_basis.shape[1]
    members, chans, lats, lon_count = predicted.shape
    degrees = legendre_basis.shape[2]
    table = jnp.asarray(fourier_table(lon_count, groups, bands, per_dev))
    rows = members * chans * lats
    far, near = reach(bands)
    basis = jnp.transpose(legendre_basis, (1, 0, 2))
    bases, slots = [basis], [0]
    step = groups // 2
    while step:
        bases = bases + [exchange(block, "batch", step) for block in bases]
        slots = slots + [slot ^ step for slot in slots]
        step //= 2

    def transform(field, staged):
        flat = field.reshape(rows, lon_count)
        if staged:
            return row_blocks(flat, table, bands, groups * per_dev * 2)
        return dft_blocks(flat, table, staged, bands, groups * per_dev * 2, chans, lats)

    first = transform(predicted, True)
    second = transform(target, False)
    got0, got1 = {0: first[0]}, {0: second[0]}
    for s in far + near:
        got0[s] = exchange(first[s], "lat", s)
        got1[s] = exchange(second[s], "lat", s)
    columns = prepared_columns([got0[s] for s in range(bands)], lats, chans)
    bases = turned_bases(bases)
    before = legendre_energy([columns], bases, slots, chans, lats, bands, [])
    blocks = [got1[s] for s in range(bands)]
    kept, sent = legendre_energy(blocks, bases, slots, chans, lats, bands, before)
    owned, other = reduce_all(kept, sent)
    spectra, loss = loss_call(
        owned, other, chans, degrees, members * groups * groups * bands * per_dev
    )
    return (jnp.transpose(spectra, (1, 0, 2)), loss.reshape(chans))


def reach(bands):
    steps = range(bands - 1, 0, -1)
    return [s for s in steps if s >= bands // 2], [s for s in steps if s < bands // 2]


def solution(mesh):
    placed = (
        P("batch", None, "lat", None),
        P("batch", None, "lat", None),
        P(None, ("batch", "lat"), None),
    )
    return jax.shard_map(spectrum_loss, mesh=mesh, in_specs=placed, out_specs=(P(), P()), check_vma=False)
```

```python
import functools
import math

import jax
import jax.numpy as jnp
import numpy as np
from jax import lax
from jax.experimental import pallas as pl
from jax.experimental.pallas import tpu as pltpu
from jax.sharding import PartitionSpec as P


LANES = 128
SPARE_VMEM = 16 * 1024 * 1024
VMEM_LIMIT = 24 * 1024 * 1024
STAGED_LIMIT = 53 * 1024 * 1024
DIRECT_LIMIT = 44 * 1024 * 1024


def round_up(value, step):
    return -(-value // step) * step


def fourier_table(lon_count, groups, bands, per_dev):
    orders = np.arange(groups * bands * per_dev).reshape(groups, bands, per_dev)
    orders = orders.transpose(1, 0, 2).reshape(-1)
    product_ids = np.arange(lon_count)[:, None] * orders[None, :] % lon_count
    angles = np.float32(2.0 * math.pi / lon_count) * product_ids.astype(np.float32)
    inv_root = np.float32(1.0 / math.sqrt(lon_count))
    both = np.stack([np.cos(angles) * inv_root, -np.sin(angles) * inv_root], axis=2)
    flat = both.reshape(lon_count, -1).astype(jnp.bfloat16)
    padded = round_up(flat.shape[1], LANES)
    return np.pad(flat, ((0, 0), (0, padded - flat.shape[1])))


def peers(count, step):
    if count & (count - 1) == 0:
        return [(i, i ^ step) for i in range(count)]
    return [(i, (i + step) % count) for i in range(count)]


def target_of(index, count, step):
    if count & (count - 1) == 0:
        return jnp.bitwise_xor(index, step)
    return lax.rem(index + step, count)


def source_of(index, count, step):
    if count & (count - 1) == 0:
        return jnp.bitwise_xor(index, step)
    return lax.rem(index + count - step, count)


def dft_kernel(bands, per, chans, lats, chunks, field, table_hbm, *rest):
    outs = rest[:bands]
    dscr, turned, packed = rest[bands : bands + 3]
    staged = len(rest) > bands + 3
    if staged:
        xbuf, table, sems = rest[bands + 3 :]
        load = pltpu.make_async_copy(table_hbm, table, sems.at[len(chunks)])
        load.start()
    else:
        xbuf, table = field, table_hbm
    copies = []
    row = 0
    for i, rows in enumerate(chunks):
        cp = None
        if staged:
            cp = pltpu.make_async_copy(
                field.at[pl.ds(row, rows), :], xbuf.at[pl.ds(row, rows), :], sems.at[i]
            )
            cp.start()
        copies.append((row, rows, cp))
        row += rows
    band = lax.axis_index("lat")
    tiles = dscr.shape[0]
    if staged:
        load.wait()
    for row, rows, cp in copies:
        if staged:
            cp.wait()
        res = jnp.dot(xbuf[pl.ds(row, rows), :], table[...], preferred_element_type=jnp.float32)
        for q in range(tiles):
            dscr[q, pl.ds(row, rows), :] = res[:, q * LANES : (q + 1) * LANES]

    def turn(q, carry):
        for n in range(lats):
            block = dscr.at[q][pl.ds(n, LANES, stride=lats), :]
            turned.at[q][pl.ds(n, LANES, stride=lats), :] = block.T
        return carry

    lax.fori_loop(0, tiles, turn, 0)

    def pack(s, carry):
        base = target_of(band, bands, s) * per
        for g in range(per):
            column = base + g
            start = pl.multiple_of(lax.rem(column, LANES) * lats, 8)
            packed[s, :, pl.ds(g * chans, chans)] = turned[
                column // LANES, pl.ds(start, lats), pl.ds(0, chans)
            ]
        return carry

    lax.fori_loop(0, bands, pack, 0, unroll=min(bands, 8))
    for s in range(bands):
        outs[s][...] = packed[s].astype(jnp.bfloat16)


def rows_kernel(bands, per, chunks, field, table_hbm, *rest):
    outs = rest[:bands]
    dscr, turned, xbuf, table, sems = rest[bands:]
    load = pltpu.make_async_copy(table_hbm, table, sems.at[len(chunks)])
    load.start()
    copies = []
    row = 0
    for i, rows in enumerate(chunks):
        cp = pltpu.make_async_copy(
            field.at[pl.ds(row, rows), :], xbuf.at[pl.ds(row, rows), :], sems.at[i]
        )
        cp.start()
        copies.append((row, rows, cp))
        row += rows
    load.wait()
    tiles = dscr.shape[0]
    for row, rows, cp in copies:
        cp.wait()
        res = jnp.dot(xbuf[pl.ds(row, rows), :], table[...], preferred_element_type=jnp.float32)
        for q in range(tiles):
            dscr[q, pl.ds(row, rows), :] = res[:, q * LANES : (q + 1) * LANES]
            for start in range(row, row + rows, LANES):
                block = dscr[q, pl.ds(start, LANES), :]
                turned[pl.ds(q * LANES, LANES), pl.ds(start, LANES)] = block.T
    band = lax.axis_index("lat")
    for s in range(bands):
        start = pl.multiple_of(target_of(band, bands, s) * per, 8)
        outs[s][...] = turned[pl.ds(start, per), :].astype(jnp.bfloat16)


def row_blocks(field, table, bands, per):
    rows_all, lon_count = field.shape
    width = round_up(rows_all, LANES)
    columns = table.shape[1]
    step = 5 * LANES
    chunks = [min(step, rows_all - row) for row in range(0, rows_all, step)]
    anywhere = pl.BlockSpec(memory_space=pl.ANY)
    vmem = pl.BlockSpec(memory_space=pltpu.VMEM)
    return pl.pallas_call(
        functools.partial(rows_kernel, bands, per, tuple(chunks)),
        out_shape=[jax.ShapeDtypeStruct((per, width), jnp.bfloat16)] * bands,
        in_specs=[anywhere] * 2,
        out_specs=[vmem] * bands,
        scratch_shapes=[
            pltpu.VMEM((columns // LANES, width, LANES), jnp.float32),
            pltpu.VMEM((columns, width), jnp.float32),
            pltpu.VMEM((rows_all, lon_count), jnp.bfloat16),
            pltpu.VMEM(table.shape, jnp.bfloat16),
            pltpu.SemaphoreType.DMA((len(chunks) + 1,)),
        ],
        compiler_params=pltpu.CompilerParams(vmem_limit_bytes=STAGED_LIMIT),
        name="dft_rows",
    )(field, table)


def dft_blocks(field, table, staged, bands, per, chans, lats):
    rows_all, lon_count = field.shape
    width = round_up(per * chans, LANES)
    step = -(-chans // 3) * lats
    chunks = []
    left = rows_all
    while left > 0:
        chunks.append(min(step, left))
        left -= step
    columns = table.shape[1]
    anywhere = pl.BlockSpec(memory_space=pl.ANY)
    vmem = pl.BlockSpec(memory_space=pltpu.VMEM)
    staging = [
        pltpu.VMEM((rows_all, lon_count), jnp.bfloat16),
        pltpu.VMEM(table.shape, jnp.bfloat16),
        pltpu.SemaphoreType.DMA((len(chunks) + 1,)),
    ]
    staging = staging if staged else []
    return pl.pallas_call(
        functools.partial(dft_kernel, bands, per, chans, lats, tuple(chunks)),
        out_shape=[jax.ShapeDtypeStruct((lats, width), jnp.bfloat16)] * bands,
        in_specs=[anywhere if staged else vmem] * 2,
        out_specs=[vmem] * bands,
        scratch_shapes=[
            pltpu.VMEM((columns // LANES, LANES * lats, LANES), jnp.float32),
            pltpu.VMEM((columns // LANES, LANES * lats, LANES), jnp.float32),
            pltpu.VMEM((bands, lats, width), jnp.float32),
        ]
        + staging,
        compiler_params=pltpu.CompilerParams(
            vmem_limit_bytes=STAGED_LIMIT if staged else DIRECT_LIMIT
        ),
        name="dft",
    )(field, table)


def turn_kernel(count, *refs):
    for basis, out in zip(refs[:count], refs[count:]):
        for o in range(basis.shape[0]):
            out[o, :, : basis.shape[1]] = basis[o].T


def turned_bases(bases):
    per_dev, lat_count, degrees = bases[0].shape
    shape = (per_dev, degrees, round_up(lat_count, LANES))
    return pl.pallas_call(
        functools.partial(turn_kernel, len(bases)),
        out_shape=[jax.ShapeDtypeStruct(shape, bases[0].dtype)] * len(bases),
        compiler_params=pltpu.CompilerParams(vmem_limit_bytes=VMEM_LIMIT),
        name="turn",
    )(*bases)


def prepare_kernel(bands, lats, chans, *refs):
    blocks, (columns, rows, flat, planes) = refs[:bands], refs[bands:]
    band = lax.axis_index("lat")
    per, width = blocks[0].shape
    fit = LANES // per
    depth = bands * lats
    for s in range(bands):
        source = source_of(band, bands, s)
        start = pl.multiple_of(source // fit * LANES + lax.rem(source, fit) * per, 8)
        rows[pl.ds(start, per), :] = blocks[s][...].astype(jnp.float32)
    tiles = flat.shape[0]
    for q in range(tiles):
        for start in range(0, width, LANES):
            block = rows[pl.ds(q * LANES, LANES), pl.ds(start, LANES)]
            flat[q, pl.ds(start, LANES), :] = block.T
    for q in range(tiles):
        for n in range(lats):
            block = flat.at[q][pl.ds(n, round_up(chans, 8), stride=lats), :].T
            for k in range(min(fit, bands - q * fit)):
                place = pl.ds((q * fit + k) * lats + n, per, stride=depth)
                planes[place, :] = jnp.pad(
                    block[k * per : (k + 1) * per, :], ((0, 0), (0, LANES - block.shape[1]))
                )
    for i in range(per // 2):
        for p in range(2):
            piece = planes[pl.ds((2 * i + p) * depth, depth), pl.ds(0, chans)]
            columns[i, :, pl.ds(p * chans, chans)] = piece.astype(jnp.bfloat16)


def prepared_columns(blocks, lats, chans):
    bands = len(blocks)
    per, width = blocks[0].shape
    tiles = -(-bands // (LANES // per))
    shape = (per // 2, bands * lats, 2 * chans)
    held = 4 * LANES * (tiles * (width + LANES * lats) + per * bands * lats)
    return pl.pallas_call(
        functools.partial(prepare_kernel, bands, lats, chans),
        out_shape=jax.ShapeDtypeStruct(shape, jnp.bfloat16),
        scratch_shapes=[
            pltpu.VMEM((tiles * LANES, width), jnp.float32),
            pltpu.VMEM((tiles, LANES * lats, LANES), jnp.float32),
            pltpu.VMEM((per * bands * lats, LANES), jnp.float32),
        ],
        compiler_params=pltpu.CompilerParams(vmem_limit_bytes=SPARE_VMEM + held),
        name="prepare",
    )(*blocks)


def energy_tiles(chans, degrees):
    lane_tiles = round_up(degrees, LANES) // LANES
    row_tiles, tail = chans // 8, chans % 8
    if tail * lane_tiles > 8:
        row_tiles, tail = row_tiles + 1, 0
    count = row_tiles * lane_tiles + (1 if tail else 0)
    return lane_tiles, row_tiles, tail, round_up(count, 4)


def legendre_kernel(bands, groups, per_dev, chans, lats, slots, field, *rest):
    inputs = bands if field else 1
    blocks = rest[:inputs]
    bases = rest[inputs : inputs + groups]
    rest = rest[inputs + groups :]
    total = rest[-1]
    if field == 0:
        out, columns = rest[0], blocks[0]
    else:
        energy_before, kept, sent, out, fourier, columns = rest[:6]
    band, group = lax.axis_index("lat"), lax.axis_index("batch")
    degrees = bases[0].shape[1]
    depth = bands * lats
    width = 2 * chans
    if field:
        for s in range(bands):
            row = pl.multiple_of(source_of(band, bands, s) * lats, 8)
            fourier[pl.ds(row, lats), :] = blocks[s][...].astype(jnp.float32)
        for i in range(groups * per_dev):
            columns[i] = fourier[:, pl.ds(i * width, width)].astype(jnp.bfloat16)
    for q in range(groups):
        owner = jnp.bitwise_xor(group, slots[q])
        first = jnp.where(jnp.logical_and(band == 0, owner == 0), 1.0, 2.0)
        squares = None
        for o in range(per_dev):
            coef = jnp.dot(
                bases[q][o, :, :depth],
                columns[owner * per_dev + o],
                preferred_element_type=jnp.float32,
            )
            term = coef * coef * (first if o == 0 else 2.0)
            squares = term if squares is None else squares + term
        if q == 0:
            total[:, pl.ds(0, width)] = squares
        else:
            total[:, pl.ds(0, width)] += squares
    sums = total[...]
    energy = sums[:, :chans] + sums[:, chans:width]
    flat = jnp.pad(
        energy, ((0, round_up(degrees, LANES) - degrees), (0, round_up(chans, 8) - chans))
    )
    lane_tiles, row_tiles, tail, count = energy_tiles(chans, degrees)
    end = row_tiles * lane_tiles
    for b in range(end, count):
        out[b] = jnp.zeros((8, LANES), jnp.float32)
    for k in range(lane_tiles):
        piece = flat[k * LANES : (k + 1) * LANES, :].T
        for r in range(row_tiles):
            out[r * lane_tiles + k] = piece[r * 8 : (r + 1) * 8, :]
        if tail:
            out[end, pl.ds(k * tail, tail), :] = piece[row_tiles * 8 : row_tiles * 8 + tail, :]
    if field == 1:
        high = lax.rem(group, 2) == 1
        first, second = energy_before[...], out[...]
        kept[...] = jnp.where(high, second, first)
        sent[...] = jnp.where(high, first, second)


def legendre_energy(blocks, bases, slots, chans, lats, bands, before):
    groups = len(bases)
    per_dev, degrees, _ = bases[0].shape
    tiles = (energy_tiles(chans, degrees)[3], 8, LANES)
    field = len(before)
    out = jax.ShapeDtypeStruct(tiles, jnp.float32)
    staging = [
        pltpu.VMEM(tiles, jnp.float32),
        pltpu.VMEM((bands * lats, blocks[0].shape[-1]), jnp.float32),
        pltpu.VMEM((groups * per_dev, bands * lats, 2 * chans), jnp.bfloat16),
    ]
    return pl.pallas_call(
        functools.partial(legendre_kernel, bands, groups, per_dev, chans, lats, slots, field),
        out_shape=[out, out] if field else [out],
        scratch_shapes=(staging if field else [])
        + [pltpu.VMEM((degrees, round_up(2 * chans, LANES)), jnp.float32)],
        compiler_params=pltpu.CompilerParams(vmem_limit_bytes=VMEM_LIMIT),
        name="legendre",
    )(*blocks, *bases, *before)


def loss_kernel(chans, degrees, count, mesh_size, *refs):
    parts = (len(refs) - 4) // 2
    owned, other = refs[:parts], refs[parts : 2 * parts]
    spectra, loss, sums, fields = refs[2 * parts :]
    lane_tiles, row_tiles, tail, _ = energy_tiles(chans, degrees)
    scale = 1.0 / count
    mine = quarter_id(mesh_size)
    high = lax.rem(lax.axis_index("batch"), 2)
    size = owned[0].shape[0]
    for m in range(parts):
        start = jnp.bitwise_xor(mine, m) * size
        fields[high, pl.ds(start, size)] = owned[m][...] * scale
        fields[1 - high, pl.ds(start, size)] = other[m][...] * scale
    for r in range(row_tiles + (1 if tail else 0)):
        rows = min(8, chans - r * 8)
        held = 8 if r < row_tiles else tail
        acc = jnp.zeros((held, LANES), jnp.float32)
        for k in range(lane_tiles):
            lanes = min(LANES, degrees - k * LANES)
            block, line = r * lane_tiles + k, 0
            if r == row_tiles:
                block, line = r * lane_tiles, k * tail
            first = fields[0, block, pl.ds(line, held), :]
            second = fields[1, block, pl.ds(line, held), :]
            spectra[pl.ds(r * 8, rows), 0, pl.ds(k * LANES, lanes)] = first[:rows, :lanes]
            spectra[pl.ds(r * 8, rows), 1, pl.ds(k * LANES, lanes)] = second[:rows, :lanes]
            gap = jnp.log(first + 1e-06) - jnp.log(second + 1e-06)
            gap = gap * gap
            if lanes < LANES:
                lane_ids = lax.broadcasted_iota(jnp.int32, gap.shape, 1)
                gap = jnp.where(lane_ids < lanes, gap, 0.0)
            acc = acc + gap
        sums[pl.ds(r * 8, held), :] = acc
    turned = sums[...].T
    loss[...] = (jnp.sum(turned, axis=0, keepdims=True) * (1.0 / degrees))[:, :chans]


def loss_call(owned, other, chans, degrees, count):
    mesh_size = lax.axis_size("batch"), lax.axis_size("lat")
    tiles = len(owned) * owned[0].shape[0]
    return pl.pallas_call(
        functools.partial(loss_kernel, chans, degrees, count, mesh_size),
        out_shape=(
            jax.ShapeDtypeStruct((chans, 2, degrees), jnp.float32),
            jax.ShapeDtypeStruct((1, chans), jnp.float32),
        ),
        scratch_shapes=[
            pltpu.VMEM((round_up(chans, 8), LANES), jnp.float32),
            pltpu.VMEM((2, tiles, 8, LANES), jnp.float32),
        ],
        compiler_params=pltpu.CompilerParams(vmem_limit_bytes=VMEM_LIMIT),
        name="loss",
    )(*owned, *other)


def exchange(value, axis, step):
    return lax.ppermute(value, axis, peers(lax.axis_size(axis), step))


def square(mesh_size):
    groups, bands = mesh_size
    return [bit for bit, there in ((1, bands > 1), (2 * bands, groups > 2)) if there]


def quarter_steps(mesh_size):
    bits = square(mesh_size)
    return [sum(bit for k, bit in enumerate(bits) if m >> k & 1) for m in range(1 << len(bits))]


def quarter_id(mesh_size):
    _, bands = mesh_size
    flat = lax.axis_index("batch") * bands + lax.axis_index("lat")
    return sum(lax.rem(flat // bit, 2) << k for k, bit in enumerate(square(mesh_size)))


def flat_exchange(value, mesh_size, step):
    count = mesh_size[0] * mesh_size[1]
    return lax.ppermute(value, ("batch", "lat"), [(i, i ^ step) for i in range(count)])


def reduce_all(kept, sent):
    mesh_size = groups, bands = lax.axis_size("batch"), lax.axis_size("lat")
    value = kept + exchange(sent, "batch", 1)
    steps = quarter_steps(mesh_size)
    mine = quarter_id(mesh_size)
    pieces = value.reshape((len(steps), value.shape[0] // len(steps)) + value.shape[1:])
    value = lax.dynamic_index_in_dim(pieces, mine, 0, keepdims=False)
    for m in range(len(steps) - 1, 0, -1):
        piece = lax.dynamic_index_in_dim(pieces, jnp.bitwise_xor(mine, m), 0, keepdims=False)
        piece = flat_exchange(piece, mesh_size, steps[m])
        value = value + piece
    step = 4
    while step < groups:
        value = value + exchange(value, "batch", step)
        step *= 2
    step = 2
    radix = 2 if bands.bit_length() % 2 == 1 else 4
    while step < bands:
        parts = [exchange(value, "lat", k * step) for k in range(radix - 1, 0, -1)]
        value = value + sum(parts[1:], parts[0])
        step *= radix
        radix = 4
    owned = [value]
    for m in range(1, len(steps)):
        owned.append(flat_exchange(value, mesh_size, steps[m]))
    return owned, [exchange(piece, "batch", 1) for piece in owned]


def spectrum_loss(predicted, target, legendre_basis):
    groups = lax.axis_size("batch")
    bands = lax.axis_size("lat")
    per_dev = legendre_basis.shape[1]
    members, chans, lats, lon_count = predicted.shape
    degrees = legendre_basis.shape[2]
    table = jnp.asarray(fourier_table(lon_count, groups, bands, per_dev))
    rows = members * chans * lats
    far, near = reach(bands)
    basis = jnp.transpose(legendre_basis, (1, 0, 2))
    bases, slots = [basis], [0]
    step = groups // 2
    while step:
        bases = bases + [exchange(block, "batch", step) for block in bases]
        slots = slots + [slot ^ step for slot in slots]
        step //= 2

    def transform(field, staged):
        flat = field.reshape(rows, lon_count)
        if staged:
            return row_blocks(flat, table, bands, groups * per_dev * 2)
        return dft_blocks(flat, table, staged, bands, groups * per_dev * 2, chans, lats)

    first = transform(predicted, True)
    second = transform(target, False)
    got0, got1 = {0: first[0]}, {0: second[0]}
    for s in far + near:
        got0[s] = exchange(first[s], "lat", s)
        got1[s] = exchange(second[s], "lat", s)
    columns = prepared_columns([got0[s] for s in range(bands)], lats, chans)
    bases = turned_bases(bases)
    before = legendre_energy([columns], bases, slots, chans, lats, bands, [])
    blocks = [got1[s] for s in range(bands)]
    kept, sent = legendre_energy(blocks, bases, slots, chans, lats, bands, before)
    owned, other = reduce_all(kept, sent)
    spectra, loss = loss_call(
        owned, other, chans, degrees, members * groups * groups * bands * per_dev
    )
    return (jnp.transpose(spectra, (1, 0, 2)), loss.reshape(chans))


def reach(bands):
    steps = range(bands - 1, 0, -1)
    return [s for s in steps if s >= bands // 2], [s for s in steps if s < bands // 2]


def solution(mesh):
    placed = (
        P("batch", None, "lat", None),
        P("batch", None, "lat", None),
        P(None, ("batch", "lat"), None),
    )
    return jax.shard_map(spectrum_loss, mesh=mesh, in_specs=placed, out_specs=(P(), P()), check_vma=False)
```

```python
import functools
import math

import jax
import jax.numpy as jnp
import numpy as np
from jax import lax
from jax.experimental import pallas as pl
from jax.experimental.pallas import tpu as pltpu
from jax.sharding import PartitionSpec as P


LANES = 128
SPARE_VMEM = 16 * 1024 * 1024
VMEM_LIMIT = 24 * 1024 * 1024
STAGED_LIMIT = 53 * 1024 * 1024
DIRECT_LIMIT = 44 * 1024 * 1024


def round_up(value, step):
    return -(-value // step) * step


def fourier_table(lon_count, groups, bands, per_dev):
    orders = np.arange(groups * bands * per_dev).reshape(groups, bands, per_dev)
    orders = orders.transpose(1, 0, 2).reshape(-1)
    product_ids = np.arange(lon_count)[:, None] * orders[None, :] % lon_count
    angles = np.float32(2.0 * math.pi / lon_count) * product_ids.astype(np.float32)
    inv_root = np.float32(1.0 / math.sqrt(lon_count))
    both = np.stack([np.cos(angles) * inv_root, -np.sin(angles) * inv_root], axis=2)
    flat = both.reshape(lon_count, -1).astype(jnp.bfloat16)
    padded = round_up(flat.shape[1], LANES)
    return np.pad(flat, ((0, 0), (0, padded - flat.shape[1])))


def peers(count, step):
    if count & (count - 1) == 0:
        return [(i, i ^ step) for i in range(count)]
    return [(i, (i + step) % count) for i in range(count)]


def target_of(index, count, step):
    if count & (count - 1) == 0:
        return jnp.bitwise_xor(index, step)
    return lax.rem(index + step, count)


def source_of(index, count, step):
    if count & (count - 1) == 0:
        return jnp.bitwise_xor(index, step)
    return lax.rem(index + count - step, count)


def dft_kernel(bands, per, chans, lats, chunks, field, table_hbm, *rest):
    outs = rest[:bands]
    dscr, turned, packed = rest[bands : bands + 3]
    staged = len(rest) > bands + 3
    if staged:
        xbuf, table, sems = rest[bands + 3 :]
        load = pltpu.make_async_copy(table_hbm, table, sems.at[len(chunks)])
        load.start()
    else:
        xbuf, table = field, table_hbm
    copies = []
    row = 0
    for i, rows in enumerate(chunks):
        cp = None
        if staged:
            cp = pltpu.make_async_copy(
                field.at[pl.ds(row, rows), :], xbuf.at[pl.ds(row, rows), :], sems.at[i]
            )
            cp.start()
        copies.append((row, rows, cp))
        row += rows
    band = lax.axis_index("lat")
    tiles = dscr.shape[0]
    if staged:
        load.wait()
    for row, rows, cp in copies:
        if staged:
            cp.wait()
        res = jnp.dot(xbuf[pl.ds(row, rows), :], table[...], preferred_element_type=jnp.float32)
        for q in range(tiles):
            dscr[q, pl.ds(row, rows), :] = res[:, q * LANES : (q + 1) * LANES]

    def turn(q, carry):
        for n in range(lats):
            block = dscr.at[q][pl.ds(n, LANES, stride=lats), :]
            turned.at[q][pl.ds(n, LANES, stride=lats), :] = block.T
        return carry

    lax.fori_loop(0, tiles, turn, 0)

    def pack(s, carry):
        base = target_of(band, bands, s) * per
        for g in range(per):
            column = base + g
            start = pl.multiple_of(lax.rem(column, LANES) * lats, 8)
            packed[s, :, pl.ds(g * chans, chans)] = turned[
                column // LANES, pl.ds(start, lats), pl.ds(0, chans)
            ]
        return carry

    lax.fori_loop(0, bands, pack, 0, unroll=min(bands, 8))
    for s in range(bands):
        outs[s][...] = packed[s].astype(jnp.bfloat16)


def rows_kernel(bands, per, chunks, field, table_hbm, *rest):
    outs = rest[:bands]
    dscr, turned, xbuf, table, sems = rest[bands:]
    load = pltpu.make_async_copy(table_hbm, table, sems.at[len(chunks)])
    load.start()
    copies = []
    row = 0
    for i, rows in enumerate(chunks):
        cp = pltpu.make_async_copy(
            field.at[pl.ds(row, rows), :], xbuf.at[pl.ds(row, rows), :], sems.at[i]
        )
        cp.start()
        copies.append((row, rows, cp))
        row += rows
    load.wait()
    tiles = dscr.shape[0]
    for row, rows, cp in copies:
        cp.wait()
        res = jnp.dot(xbuf[pl.ds(row, rows), :], table[...], preferred_element_type=jnp.float32)
        for q in range(tiles):
            dscr[q, pl.ds(row, rows), :] = res[:, q * LANES : (q + 1) * LANES]
            for start in range(row, row + rows, LANES):
                block = dscr[q, pl.ds(start, LANES), :]
                turned[pl.ds(q * LANES, LANES), pl.ds(start, LANES)] = block.T
    band = lax.axis_index("lat")
    for s in range(bands):
        start = pl.multiple_of(target_of(band, bands, s) * per, 8)
        outs[s][...] = turned[pl.ds(start, per), :].astype(jnp.bfloat16)


def row_blocks(field, table, bands, per):
    rows_all, lon_count = field.shape
    width = round_up(rows_all, LANES)
    columns = table.shape[1]
    step = 6 * LANES
    chunks = [min(step, rows_all - row) for row in range(0, rows_all, step)]
    anywhere = pl.BlockSpec(memory_space=pl.ANY)
    vmem = pl.BlockSpec(memory_space=pltpu.VMEM)
    return pl.pallas_call(
        functools.partial(rows_kernel, bands, per, tuple(chunks)),
        out_shape=[jax.ShapeDtypeStruct((per, width), jnp.bfloat16)] * bands,
        in_specs=[anywhere] * 2,
        out_specs=[vmem] * bands,
        scratch_shapes=[
            pltpu.VMEM((columns // LANES, width, LANES), jnp.float32),
            pltpu.VMEM((columns, width), jnp.float32),
            pltpu.VMEM((rows_all, lon_count), jnp.bfloat16),
            pltpu.VMEM(table.shape, jnp.bfloat16),
            pltpu.SemaphoreType.DMA((len(chunks) + 1,)),
        ],
        compiler_params=pltpu.CompilerParams(vmem_limit_bytes=STAGED_LIMIT),
        name="dft_rows",
    )(field, table)


def dft_blocks(field, table, staged, bands, per, chans, lats):
    rows_all, lon_count = field.shape
    width = round_up(per * chans, LANES)
    step = -(-chans // 3) * lats
    chunks = []
    left = rows_all
    while left > 0:
        chunks.append(min(step, left))
        left -= step
    columns = table.shape[1]
    anywhere = pl.BlockSpec(memory_space=pl.ANY)
    vmem = pl.BlockSpec(memory_space=pltpu.VMEM)
    staging = [
        pltpu.VMEM((rows_all, lon_count), jnp.bfloat16),
        pltpu.VMEM(table.shape, jnp.bfloat16),
        pltpu.SemaphoreType.DMA((len(chunks) + 1,)),
    ]
    staging = staging if staged else []
    return pl.pallas_call(
        functools.partial(dft_kernel, bands, per, chans, lats, tuple(chunks)),
        out_shape=[jax.ShapeDtypeStruct((lats, width), jnp.bfloat16)] * bands,
        in_specs=[anywhere if staged else vmem] * 2,
        out_specs=[vmem] * bands,
        scratch_shapes=[
            pltpu.VMEM((columns // LANES, LANES * lats, LANES), jnp.float32),
            pltpu.VMEM((columns // LANES, LANES * lats, LANES), jnp.float32),
            pltpu.VMEM((bands, lats, width), jnp.float32),
        ]
        + staging,
        compiler_params=pltpu.CompilerParams(
            vmem_limit_bytes=STAGED_LIMIT if staged else DIRECT_LIMIT
        ),
        name="dft",
    )(field, table)


def turn_kernel(count, *refs):
    for basis, out in zip(refs[:count], refs[count:]):
        for o in range(basis.shape[0]):
            out[o, :, : basis.shape[1]] = basis[o].T


def turned_bases(bases):
    per_dev, lat_count, degrees = bases[0].shape
    shape = (per_dev, degrees, round_up(lat_count, LANES))
    return pl.pallas_call(
        functools.partial(turn_kernel, len(bases)),
        out_shape=[jax.ShapeDtypeStruct(shape, bases[0].dtype)] * len(bases),
        compiler_params=pltpu.CompilerParams(vmem_limit_bytes=VMEM_LIMIT),
        name="turn",
    )(*bases)


def prepare_kernel(bands, lats, chans, *refs):
    blocks, (columns, rows, flat, planes) = refs[:bands], refs[bands:]
    band = lax.axis_index("lat")
    per, width = blocks[0].shape
    fit = LANES // per
    depth = bands * lats
    for s in range(bands):
        source = source_of(band, bands, s)
        start = pl.multiple_of(source // fit * LANES + lax.rem(source, fit) * per, 8)
        rows[pl.ds(start, per), :] = blocks[s][...].astype(jnp.float32)
    tiles = flat.shape[0]
    for q in range(tiles):
        for start in range(0, width, LANES):
            block = rows[pl.ds(q * LANES, LANES), pl.ds(start, LANES)]
            flat[q, pl.ds(start, LANES), :] = block.T
    for q in range(tiles):
        for n in range(lats):
            block = flat.at[q][pl.ds(n, round_up(chans, 8), stride=lats), :].T
            for k in range(min(fit, bands - q * fit)):
                place = pl.ds((q * fit + k) * lats + n, per, stride=depth)
                planes[place, :] = jnp.pad(
                    block[k * per : (k + 1) * per, :], ((0, 0), (0, LANES - block.shape[1]))
                )
    for i in range(per // 2):
        for p in range(2):
            piece = planes[pl.ds((2 * i + p) * depth, depth), pl.ds(0, chans)]
            columns[i, :, pl.ds(p * chans, chans)] = piece.astype(jnp.bfloat16)


def prepared_columns(blocks, lats, chans):
    bands = len(blocks)
    per, width = blocks[0].shape
    tiles = -(-bands // (LANES // per))
    shape = (per // 2, bands * lats, 2 * chans)
    held = 4 * LANES * (tiles * (width + LANES * lats) + per * bands * lats)
    return pl.pallas_call(
        functools.partial(prepare_kernel, bands, lats, chans),
        out_shape=jax.ShapeDtypeStruct(shape, jnp.bfloat16),
        scratch_shapes=[
            pltpu.VMEM((tiles * LANES, width), jnp.float32),
            pltpu.VMEM((tiles, LANES * lats, LANES), jnp.float32),
            pltpu.VMEM((per * bands * lats, LANES), jnp.float32),
        ],
        compiler_params=pltpu.CompilerParams(vmem_limit_bytes=SPARE_VMEM + held),
        name="prepare",
    )(*blocks)


def energy_tiles(chans, degrees):
    lane_tiles = round_up(degrees, LANES) // LANES
    row_tiles, tail = chans // 8, chans % 8
    if tail * lane_tiles > 8:
        row_tiles, tail = row_tiles + 1, 0
    count = row_tiles * lane_tiles + (1 if tail else 0)
    return lane_tiles, row_tiles, tail, round_up(count, 4)


def legendre_kernel(bands, groups, per_dev, chans, lats, slots, field, *rest):
    inputs = bands if field else 1
    blocks = rest[:inputs]
    bases = rest[inputs : inputs + groups]
    rest = rest[inputs + groups :]
    total = rest[-1]
    if field == 0:
        out, columns = rest[0], blocks[0]
    else:
        energy_before, kept, sent, out, fourier, columns = rest[:6]
    band, group = lax.axis_index("lat"), lax.axis_index("batch")
    degrees = bases[0].shape[1]
    depth = bands * lats
    width = 2 * chans
    if field:
        for s in range(bands):
            row = pl.multiple_of(source_of(band, bands, s) * lats, 8)
            fourier[pl.ds(row, lats), :] = blocks[s][...].astype(jnp.float32)
        for i in range(groups * per_dev):
            columns[i] = fourier[:, pl.ds(i * width, width)].astype(jnp.bfloat16)
    for q in range(groups):
        owner = jnp.bitwise_xor(group, slots[q])
        first = jnp.where(jnp.logical_and(band == 0, owner == 0), 1.0, 2.0)
        squares = None
        for o in range(per_dev):
            coef = jnp.dot(
                bases[q][o, :, :depth],
                columns[owner * per_dev + o],
                preferred_element_type=jnp.float32,
            )
            term = coef * coef * (first if o == 0 else 2.0)
            squares = term if squares is None else squares + term
        if q == 0:
            total[:, pl.ds(0, width)] = squares
        else:
            total[:, pl.ds(0, width)] += squares
    sums = total[...]
    energy = sums[:, :chans] + sums[:, chans:width]
    flat = jnp.pad(
        energy, ((0, round_up(degrees, LANES) - degrees), (0, round_up(chans, 8) - chans))
    )
    lane_tiles, row_tiles, tail, count = energy_tiles(chans, degrees)
    end = row_tiles * lane_tiles
    for b in range(end, count):
        out[b] = jnp.zeros((8, LANES), jnp.float32)
    for k in range(lane_tiles):
        piece = flat[k * LANES : (k + 1) * LANES, :].T
        for r in range(row_tiles):
            out[r * lane_tiles + k] = piece[r * 8 : (r + 1) * 8, :]
        if tail:
            out[end, pl.ds(k * tail, tail), :] = piece[row_tiles * 8 : row_tiles * 8 + tail, :]
    if field == 1:
        high = lax.rem(group, 2) == 1
        first, second = energy_before[...], out[...]
        kept[...] = jnp.where(high, second, first)
        sent[...] = jnp.where(high, first, second)


def legendre_energy(blocks, bases, slots, chans, lats, bands, before):
    groups = len(bases)
    per_dev, degrees, _ = bases[0].shape
    tiles = (energy_tiles(chans, degrees)[3], 8, LANES)
    field = len(before)
    out = jax.ShapeDtypeStruct(tiles, jnp.float32)
    staging = [
        pltpu.VMEM(tiles, jnp.float32),
        pltpu.VMEM((bands * lats, blocks[0].shape[-1]), jnp.float32),
        pltpu.VMEM((groups * per_dev, bands * lats, 2 * chans), jnp.bfloat16),
    ]
    return pl.pallas_call(
        functools.partial(legendre_kernel, bands, groups, per_dev, chans, lats, slots, field),
        out_shape=[out, out] if field else [out],
        scratch_shapes=(staging if field else [])
        + [pltpu.VMEM((degrees, round_up(2 * chans, LANES)), jnp.float32)],
        compiler_params=pltpu.CompilerParams(vmem_limit_bytes=VMEM_LIMIT),
        name="legendre",
    )(*blocks, *bases, *before)


def loss_kernel(chans, degrees, count, mesh_size, *refs):
    parts = (len(refs) - 4) // 2
    owned, other = refs[:parts], refs[parts : 2 * parts]
    spectra, loss, sums, fields = refs[2 * parts :]
    lane_tiles, row_tiles, tail, _ = energy_tiles(chans, degrees)
    scale = 1.0 / count
    mine = quarter_id(mesh_size)
    high = lax.rem(lax.axis_index("batch"), 2)
    size = owned[0].shape[0]
    for m in range(parts):
        start = jnp.bitwise_xor(mine, m) * size
        fields[high, pl.ds(start, size)] = owned[m][...] * scale
        fields[1 - high, pl.ds(start, size)] = other[m][...] * scale
    for r in range(row_tiles + (1 if tail else 0)):
        rows = min(8, chans - r * 8)
        held = 8 if r < row_tiles else tail
        acc = jnp.zeros((held, LANES), jnp.float32)
        for k in range(lane_tiles):
            lanes = min(LANES, degrees - k * LANES)
            block, line = r * lane_tiles + k, 0
            if r == row_tiles:
                block, line = r * lane_tiles, k * tail
            first = fields[0, block, pl.ds(line, held), :]
            second = fields[1, block, pl.ds(line, held), :]
            spectra[pl.ds(r * 8, rows), 0, pl.ds(k * LANES, lanes)] = first[:rows, :lanes]
            spectra[pl.ds(r * 8, rows), 1, pl.ds(k * LANES, lanes)] = second[:rows, :lanes]
            gap = jnp.log(first + 1e-06) - jnp.log(second + 1e-06)
            gap = gap * gap
            if lanes < LANES:
                lane_ids = lax.broadcasted_iota(jnp.int32, gap.shape, 1)
                gap = jnp.where(lane_ids < lanes, gap, 0.0)
            acc = acc + gap
        sums[pl.ds(r * 8, held), :] = acc
    turned = sums[...].T
    loss[...] = (jnp.sum(turned, axis=0, keepdims=True) * (1.0 / degrees))[:, :chans]


def loss_call(owned, other, chans, degrees, count):
    mesh_size = lax.axis_size("batch"), lax.axis_size("lat")
    tiles = len(owned) * owned[0].shape[0]
    return pl.pallas_call(
        functools.partial(loss_kernel, chans, degrees, count, mesh_size),
        out_shape=(
            jax.ShapeDtypeStruct((chans, 2, degrees), jnp.float32),
            jax.ShapeDtypeStruct((1, chans), jnp.float32),
        ),
        scratch_shapes=[
            pltpu.VMEM((round_up(chans, 8), LANES), jnp.float32),
            pltpu.VMEM((2, tiles, 8, LANES), jnp.float32),
        ],
        compiler_params=pltpu.CompilerParams(vmem_limit_bytes=VMEM_LIMIT),
        name="loss",
    )(*owned, *other)


def exchange(value, axis, step):
    return lax.ppermute(value, axis, peers(lax.axis_size(axis), step))


def square(mesh_size):
    groups, bands = mesh_size
    return [bit for bit, there in ((1, bands > 1), (2 * bands, groups > 2)) if there]


def quarter_steps(mesh_size):
    bits = square(mesh_size)
    return [sum(bit for k, bit in enumerate(bits) if m >> k & 1) for m in range(1 << len(bits))]


def quarter_id(mesh_size):
    _, bands = mesh_size
    flat = lax.axis_index("batch") * bands + lax.axis_index("lat")
    return sum(lax.rem(flat // bit, 2) << k for k, bit in enumerate(square(mesh_size)))


def flat_exchange(value, mesh_size, step):
    count = mesh_size[0] * mesh_size[1]
    return lax.ppermute(value, ("batch", "lat"), [(i, i ^ step) for i in range(count)])


def band_stages(bands):
    stages, step = [], 2
    radix = 2 if bands.bit_length() % 2 == 1 else 4
    while step < bands:
        stages.append([k * step for k in sorted(range(1, radix), key=lambda k: (k == 1, k))])
        step *= radix
        radix = 4
    return stages


def reduce_all(kept, sent):
    mesh_size = groups, bands = lax.axis_size("batch"), lax.axis_size("lat")
    value = kept + exchange(sent, "batch", 1)
    steps = quarter_steps(mesh_size)
    mine = quarter_id(mesh_size)
    pieces = value.reshape((len(steps), value.shape[0] // len(steps)) + value.shape[1:])
    value = lax.dynamic_index_in_dim(pieces, mine, 0, keepdims=False)
    for m in range(len(steps) - 1, 0, -1):
        piece = lax.dynamic_index_in_dim(pieces, jnp.bitwise_xor(mine, m), 0, keepdims=False)
        piece = flat_exchange(piece, mesh_size, steps[m])
        value = value + piece
    step = 4
    while step < groups:
        value = value + exchange(value, "batch", step)
        step *= 2
    for distances in band_stages(bands):
        parts = []
        for distance in distances:
            parts.append(exchange(value, "lat", distance))
        value = value + sum(parts[1:], parts[0])
    owned = [value]
    for m in range(1, len(steps)):
        owned.append(flat_exchange(value, mesh_size, steps[m]))
    return owned, [exchange(piece, "batch", 1) for piece in owned]


def spectrum_loss(predicted, target, legendre_basis):
    groups = lax.axis_size("batch")
    bands = lax.axis_size("lat")
    per_dev = legendre_basis.shape[1]
    members, chans, lats, lon_count = predicted.shape
    degrees = legendre_basis.shape[2]
    table = jnp.asarray(fourier_table(lon_count, groups, bands, per_dev))
    rows = members * chans * lats
    far, near = reach(bands)
    basis = jnp.transpose(legendre_basis, (1, 0, 2))
    bases, slots = [basis], [0]
    step = groups // 2
    while step:
        bases = bases + [exchange(block, "batch", step) for block in bases]
        slots = slots + [slot ^ step for slot in slots]
        step //= 2

    def transform(field, staged):
        flat = field.reshape(rows, lon_count)
        if staged:
            return row_blocks(flat, table, bands, groups * per_dev * 2)
        return dft_blocks(flat, table, staged, bands, groups * per_dev * 2, chans, lats)

    first = transform(predicted, True)
    second = transform(target, False)
    got0, got1 = {0: first[0]}, {0: second[0]}
    for s in far + near:
        got0[s] = exchange(first[s], "lat", s)
        got1[s] = exchange(second[s], "lat", s)
    columns = prepared_columns([got0[s] for s in range(bands)], lats, chans)
    bases = turned_bases(bases)
    before = legendre_energy([columns], bases, slots, chans, lats, bands, [])
    blocks = [got1[s] for s in range(bands)]
    kept, sent = legendre_energy(blocks, bases, slots, chans, lats, bands, before)
    owned, other = reduce_all(kept, sent)
    spectra, loss = loss_call(
        owned, other, chans, degrees, members * groups * groups * bands * per_dev
    )
    return (jnp.transpose(spectra, (1, 0, 2)), loss.reshape(chans))


def reach(bands):
    steps = range(bands - 1, 0, -1)
    return [s for s in steps if s >= bands // 2], [s for s in steps if s < bands // 2]


def solution(mesh):
    placed = (
        P("batch", None, "lat", None),
        P("batch", None, "lat", None),
        P(None, ("batch", "lat"), None),
    )
    return jax.shard_map(spectrum_loss, mesh=mesh, in_specs=placed, out_specs=(P(), P()), check_vma=False)
```
